32 devices in a mesh: gx: 4 (over z), gy: 8 (over y, x, core).
Axes of the slice: x: 2, y: 2, z: 4, core: 2. Of those that a mesh axis runs over, the one named last changes fastest.
Arguments:
- conductivity: float32 [128, 32768], P(('gx', 'gy')), may hold values from 0.5 to 2
- owner_rank: int32 [8192, 1], P(('gx', 'gy')), may hold values from 0 to 31; in each aligned block of 256 rows (0 to 255, 256 to 511, ...) at most 17 rows name the same one
- tile_slot: int32 [8192], P(('gx', 'gy')), may hold values from 0 to 3
- offsets: int32 [3, 8192], P(None, ('gx', 'gy')), may hold values from 0 to 30
- fractions: float32 [3, 8192], P(None, ('gx', 'gy')), may hold values from 0 to 1
- source: float32 [8192], P(('gx', 'gy')), may hold values from -1.5 to 1.5
- observed: float32 [8192], P(('gx', 'gy')), may hold values from -3 to 3
- live_count: int32 [32], P(('gx', 'gy')), may hold values from 1 to 256, 6144 in all
- fourier: float32 [128, 3], replicated, may hold values from -1.5 to 1.5
- weights: float32 [6, 256, 256], replicated, may hold values from -0.375 to 0.375
- biases: float32 [6, 256], replicated, may hold values from -3 to 3
- readout: float32 [256], replicated, may hold values from -0.375 to 0.375
Outputs:
- conductivity_grad: float32 [128, 32768], P(('gx', 'gy'))
- weight_grad: float32 [6, 256, 256], replicated
- bias_grad: float32 [6, 256], replicated
- readout_grad: float32 [256], replicated
- losses: float32 [3], replicated
The draws below stay inside these ranges and needn't reach their ends.
Inputs may be any that keep to these rules, and one draw needn't show every extreme that they name: `owner_rank`: among the rows of one device at most 17 name the same owner, and that number is reached in some device's rows. `live_count`: they sum to 6144, and some device has all 256 points live.
All inputs are finite; a program needn't handle non-finite values.
Results may differ from the reference program's by a relative error of at most 0.0003.
Values sent between devices are 32-bit elements; how exact they have to be, the bound alone decides.
No kernel may reach another device: no remote copies, remote signals or barrier semaphores. Data moves between devices by JAX's collectives and lax.ppermute only.
A program may use at most 128 MiB of HBM per device.

```python
import math
import jax
import jax.numpy as jnp
import numpy as np
from jax import lax

TILE_SIDE = 32
TILES_DEV = 4
POINTS_DEV = 256
WIDTH = 256
LAYERS = 6
FREQS = 128
CELLS = 32768
TILES = 128
POINTS = 8192
CAP = 17
DEVICES = 32


def set_ends(result, key, smallest, top_value):
    longest = result.shape.index(max(result.shape))
    spots = []
    for shift in (0, 1):
        where = [jax.random.randint(jax.random.fold_in(key, axis), (), 0, length) for axis, length in enumerate(result.shape)]
        where[longest] = (where[longest] + shift) % result.shape[longest]
        spots.append(tuple(where))
    return result.at[spots[0]].set(smallest).at[spots[1]].set(top_value)


def steps_of(stream_key, dims, cuts, least, top_value):
    def one(axis_at, shards_of):
        steps = jax.random.uniform(jax.random.fold_in(jax.random.fold_in(stream_key, 6), axis_at), (shards_of,), jnp.float32, least / len(cuts), top_value / len(cuts))
        return jnp.repeat(jnp.exp(steps), dims[axis_at] // shards_of).reshape((-1,) + (1,) * (len(dims) - axis_at - 1))

    factor_of = one(*cuts[0])
    for cut in cuts[1:]:
        factor_of = factor_of * one(*cut)
    return factor_of


def profile(count, total, bound, slope):
    portions = [(1 << 20) // math.isqrt(standing ** slope) + 1 for standing in range(2, count + 1)]
    surplus, holding = total - bound - (count - 1), [1] * (count - 1)
    while surplus > 0:
        movable = [i for i in range(count - 1) if holding[i] < bound]
        pool, left = sum([portions[i] for i in movable]), surplus
        for i in movable:
            addition = min(bound - holding[i], max(1, left * portions[i] // pool), surplus)
            holding[i] = holding[i] + addition
            surplus = surplus - addition
    return np.array([bound] + holding)


def ragged_sizes(rng, amount, total, reach, slope):
    if amount == 2:
        one = jax.random.randint(rng, (), max(1, total - reach), min(reach, total - 1) + 1)
        return jnp.stack([one, total - one])
    lengths = jnp.asarray(profile(amount, total, reach, slope), jnp.int32)
    twos = (amount - 1) // 2
    donor, receiver = lengths[1:1 + 2 * twos:2], lengths[2:2 + 2 * twos:2]
    room = jnp.minimum(donor - 1, reach - receiver)
    shifted = jax.random.randint(jax.random.fold_in(rng, 1), (twos,), 0, 1 << 20) % (room + 1)
    lengths = lengths.at[1:1 + 2 * twos:2].set(donor - shifted).at[2:2 + 2 * twos:2].set(receiver + shifted)
    return lengths[jax.random.permutation(jax.random.fold_in(rng, 2), amount)]


def shared_out(stream_key, own, number, rows, number_of, top, reach, lean):
    sequence = jax.random.permutation(stream_key, number_of)
    heavy_load, common = shares(number_of, rows * top, reach, lean, True), shares(number_of, rows * top, reach, lean, False)
    places = jnp.arange(number_of)

    def named(sizes, offset_by):
        used = int((sizes > 0).sum())
        fixed = max(1, used // 4)
        shifted = fixed + (places - fixed + offset_by * (used - fixed)) % max(1, number_of - fixed)
        return jnp.zeros((number_of,), jnp.int32).at[sequence[jnp.where(places < fixed, places, shifted)]].set(jnp.asarray(sizes, jnp.int32))

    sizes = jnp.where(number % 4 == 0, named(heavy_load, number // 4), named(common, number - number // 4 - 1))
    mixed = jax.random.permutation(jax.random.fold_in(own, 3), number_of)
    donor, taker = mixed[0:number_of // 2 * 2:2], mixed[1:number_of // 2 * 2:2]
    margin = jnp.minimum(sizes[donor] - 1, reach - sizes[taker]) // 2
    margin = jnp.where((donor == sequence[0]) | (taker == sequence[0]) | (sizes[taker] == 0), 0, jnp.maximum(margin, 0))
    shifted = jax.random.randint(jax.random.fold_in(own, 4), (number_of // 2,), 0, 1 << 20) % (margin + 1)
    sizes = sizes.at[donor].add(-shifted).at[taker].add(shifted)
    items = jnp.searchsorted(jnp.cumsum(sizes), jnp.arange(rows * top), side="right").astype(jnp.int32)
    listing = items.reshape(top, rows).T
    listing = listing[jax.random.permutation(jax.random.fold_in(own, 1), rows)]
    offset_by = jax.random.randint(jax.random.fold_in(own, 2), (rows, 1), 0, top)
    return jnp.take_along_axis(listing, (jnp.arange(top)[None, :] + offset_by) % top, axis=1)


def shares(amount, total, bound, skew, full):
    portions = [(1 << 20) // math.isqrt(grade ** skew) + 1 for grade in range(1, amount + 1)]
    largest = bound if full else min(bound, max(-(-total // amount), total * portions[0] // sum(portions)))
    least = 1 if total - largest >= amount - 1 else 0
    holding, surplus = [largest] + [least] * (amount - 1), total - largest - least * (amount - 1)
    while surplus > 0:
        candidates = [i for i in range(1, amount) if holding[i] < largest] or [i for i in range(1, amount) if holding[i] < bound]
        whole, remaining = sum([portions[i] for i in candidates]), surplus
        for i in candidates:
            addition = min(bound - holding[i], max(1, remaining * portions[i] // whole), surplus)
            holding[i] = holding[i] + addition
            surplus = surplus - addition
    return np.array(holding)


def gaussian(key, extent, deviation, most, pieces=(), kind=jnp.bfloat16):
    result = deviation * jax.random.normal(key, extent, jnp.float32)
    if pieces:
        result = result * steps_of(key, extent, pieces, -0.22, 0.18)
    return jnp.clip(result, -most, most).astype(kind)


def setup_inputs(seed: int = 0) -> dict:
    key_list = jax.random.split(jax.random.key(seed), 13)
    conductivity = jnp.clip(jnp.exp(math.log(2.0) - 1.3862944 * jax.random.uniform(key_list[0], (TILES, CELLS), jnp.float32) ** steps_of(key_list[0], (TILES, CELLS), ((0, 32),), -0.2, 0.2)), 0.5, 2.0)
    owner_rank_keys = jax.random.split(jax.random.fold_in(key_list[1], 1), POINTS // POINTS_DEV)
    owner_rank_turns = jax.random.permutation(jax.random.fold_in(key_list[1], 3), POINTS // POINTS_DEV)
    owner_rank = jax.vmap(lambda own, number: shared_out(jax.random.fold_in(key_list[1], 2), own, number, POINTS_DEV, DEVICES, 1, CAP, 2))(owner_rank_keys, owner_rank_turns).reshape((POINTS, 1))
    tile_slot = set_ends(jax.random.randint(key_list[2], (POINTS,), 0, TILES_DEV), jax.random.fold_in(key_list[2], 1), 0, TILES_DEV - 1).astype(jnp.int32)
    offsets = set_ends(jax.random.randint(key_list[3], (3, POINTS), 0, TILE_SIDE - 1), jax.random.fold_in(key_list[3], 1), 0, (TILE_SIDE - 1) - 1).astype(jnp.int32)
    fractions = jnp.clip(1.0 * jax.random.uniform(key_list[4], (3, POINTS), jnp.float32) ** steps_of(key_list[4], (3, POINTS), ((1, 32),), -0.2, 0.2), 0.0, 1.0)
    source = gaussian(key_list[5], (POINTS,), 0.25, 1.5, ((0, 32),), jnp.float32)
    observed = gaussian(key_list[6], (POINTS,), 0.5, 3.0, ((0, 32),), jnp.float32)
    live_count = ragged_sizes(key_list[7], DEVICES, 3 * POINTS // 4, POINTS_DEV, 2).astype(jnp.int32)
    fourier = gaussian(key_list[8], (FREQS, 3), 0.25, 1.5, (), jnp.float32)
    weights = gaussian(key_list[9], (LAYERS, WIDTH, WIDTH), WIDTH ** -0.5, 0.375, (), jnp.float32)
    biases = gaussian(key_list[10], (LAYERS, WIDTH), 0.5, 3.0, (), jnp.float32)
    readout = gaussian(key_list[11], (WIDTH,), WIDTH ** -0.5, 0.375, (), jnp.float32)
    return {"conductivity": conductivity, "owner_rank": owner_rank, "tile_slot": tile_slot, "offsets": offsets, "fractions": fractions, "source": source, "observed": observed, "live_count": live_count, "fourier": fourier, "weights": weights, "biases": biases, "readout": readout}


data_weight = 1.0
smooth_weight = 0.05
highest = lax.Precision.HIGHEST

def encode(fourier, position):
    phases = fourier[:, 0:1] * position[0][None, :] + fourier[:, 1:2] * position[1][None, :] + fourier[:, 2:3] * position[2][None, :]
    sin_part = jnp.sin(phases)
    cos_part = jnp.cos(phases)
    squared = lax.optimization_barrier(jnp.sum(fourier * fourier, axis=1, keepdims=True))
    streams = [jnp.concatenate([sin_part, cos_part], axis=0)]
    for column in range(3):
        column_rate = fourier[:, column:column + 1]
        streams.append(jnp.concatenate([cos_part * column_rate, -sin_part * column_rate], axis=0))
    streams.append(jnp.concatenate([-sin_part * squared, -cos_part * squared], axis=0))
    return jnp.stack(streams)

def hidden_layer(weight, bias_row, streams):
    projected = jnp.einsum('oi,sip->sop', weight, streams, precision=highest)
    values = jnp.tanh(projected[0] + bias_row[:, None])
    slopes = 1.0 - values * values
    gradient_part = slopes[None] * projected[1:4]
    curvature = slopes * projected[4] - 2.0 * values * slopes * lax.optimization_barrier(jnp.sum(projected[1:4] * projected[1:4], axis=0))
    return jnp.concatenate([values[None], gradient_part, curvature[None]], axis=0)

def readout_map(readout, streams):
    return jnp.einsum('i,sip->sp', readout, streams, precision=highest)

def network(weights, biases, readout, fourier, position):
    streams = encode(fourier, position)
    for layer_depth in range(LAYERS):
        streams = hidden_layer(weights[layer_depth], biases[layer_depth], streams)
    return readout_map(readout, streams)

def point_objective(weights, biases, readout, point_values, fourier, position, source, observed, live_mask):
    outputs = network(weights, biases, readout, fourier, position)
    residual = -(point_values[0] * outputs[4] + lax.optimization_barrier(jnp.sum(point_values[1:4] * outputs[1:4], axis=0))) - source
    misfit = outputs[0] - observed
    residual_sum = jnp.sum(live_mask * residual * residual)
    misfit_sum = jnp.sum(live_mask * misfit * misfit)
    return (residual_sum + data_weight * misfit_sum, (residual_sum, misfit_sum))

def interpolate(flat_field, cell_index, fractions):
    lower_weight = 1.0 - fractions
    value_sum = jnp.zeros_like(fractions[0])
    first_sum = jnp.zeros_like(fractions[0])
    second_sum = jnp.zeros_like(fractions[0])
    third_sum = jnp.zeros_like(fractions[0])
    for along_x in (0, 1):
        for along_y in (0, 1):
            for along_z in (0, 1):
                shift_cells = (along_x * TILE_SIDE + along_y) * TILE_SIDE + along_z
                corner = flat_field[cell_index + shift_cells]
                weight_first = fractions[0] if along_x else lower_weight[0]
                weight_second = fractions[1] if along_y else lower_weight[1]
                weight_third = fractions[2] if along_z else lower_weight[2]
                sign_first = 1.0 if along_x else -1.0
                sign_second = 1.0 if along_y else -1.0
                sign_third = 1.0 if along_z else -1.0
                value_sum = value_sum + weight_first * weight_second * weight_third * corner
                first_sum = first_sum + sign_first * weight_second * weight_third * corner
                second_sum = second_sum + weight_first * sign_second * weight_third * corner
                third_sum = third_sum + weight_first * weight_second * sign_third * corner
    return jnp.stack([value_sum, first_sum, second_sum, third_sum])

def spread(size, cell_index, fractions, gradient_rows):
    lower_weight = 1.0 - fractions
    accumulated = jnp.zeros((size,), gradient_rows.dtype)
    for along_x in (0, 1):
        for along_y in (0, 1):
            for along_z in (0, 1):
                shift_cells = (along_x * TILE_SIDE + along_y) * TILE_SIDE + along_z
                weight_first = fractions[0] if along_x else lower_weight[0]
                weight_second = fractions[1] if along_y else lower_weight[1]
                weight_third = fractions[2] if along_z else lower_weight[2]
                sign_first = 1.0 if along_x else -1.0
                sign_second = 1.0 if along_y else -1.0
                sign_third = 1.0 if along_z else -1.0
                contribution = gradient_rows[0] * weight_first * weight_second * weight_third + gradient_rows[1] * sign_first * weight_second * weight_third + gradient_rows[2] * weight_first * sign_second * weight_third + gradient_rows[3] * weight_first * weight_second * sign_third
                accumulated = accumulated.at[cell_index + shift_cells].add(contribution)
    return accumulated

def smooth_field(conductivity, row_count):
    tile_side = TILE_SIDE
    tiles_per_row = conductivity.shape[0] // row_count
    field_grid = conductivity.reshape(row_count, tiles_per_row, tile_side, tile_side, tile_side)
    field_grid = field_grid.transpose(0, 3, 1, 2, 4).reshape(row_count * tile_side, tiles_per_row * tile_side, tile_side)
    energy = jnp.zeros((), field_grid.dtype)
    gradient = jnp.zeros_like(field_grid)
    for direction in range(3):
        difference = jnp.diff(field_grid, axis=direction)
        energy = energy + jnp.sum(difference * difference)
        pad_before = [(0, 0), (0, 0), (0, 0)]
        pad_after = [(0, 0), (0, 0), (0, 0)]
        pad_before[direction] = (1, 0)
        pad_after[direction] = (0, 1)
        gradient = gradient + jnp.pad(difference, pad_before) - jnp.pad(difference, pad_after)
    gradient = 2.0 * smooth_weight * gradient
    gradient = gradient.reshape(row_count, tile_side, tiles_per_row, tile_side, tile_side)
    gradient = gradient.transpose(0, 2, 3, 1, 4).reshape(conductivity.shape)
    return (energy, gradient)

def reference(conductivity, owner_rank, tile_slot, offsets, fractions, source, observed, live_count, fourier, weights, biases, readout):
    blocks = live_count.shape[0]
    point_count = tile_slot.shape[0]
    block_points = point_count // blocks
    tile_cells = TILE_SIDE ** 3
    owner_device = owner_rank[:, 0]
    tile_index = owner_device * (conductivity.shape[0] // blocks) + tile_slot
    cell_index = (tile_index * tile_cells + (offsets[0] * TILE_SIDE + offsets[1]) * TILE_SIDE + offsets[2]).astype(jnp.int32)
    flat_field = conductivity.reshape(-1)
    point_values = interpolate(flat_field, cell_index, fractions)
    position = jnp.stack([TILE_SIDE * tile_slot + offsets[0], TILE_SIDE * owner_device + offsets[1], offsets[2]]).astype(jnp.float32) + fractions
    point_order = lax.broadcasted_iota(jnp.int32, (point_count,), 0)
    live_mask = (point_order % block_points < live_count[point_order // block_points]).astype(jnp.float32)

    def split_blocks(stacked):
        return stacked.reshape(stacked.shape[0], blocks, block_points).transpose(1, 0, 2)
    inputs = (split_blocks(point_values), split_blocks(position), source.reshape(blocks, block_points), observed.reshape(blocks, block_points), live_mask.reshape(blocks, block_points))

    def per_block(running, block_data):
        values, position_rows, forcing, target, mask_row = block_data

        def objective(weight_stack, bias_stack, readout_row, value_rows):
            return point_objective(weight_stack, bias_stack, readout_row, value_rows, fourier, position_rows, forcing, target, mask_row)
        objective_value, pull_back, partial_sums = jax.vjp(objective, weights, biases, readout, values, has_aux=True)
        grad_weight, grad_bias, grad_readout, grad_values = pull_back(jnp.ones_like(objective_value))
        running = (running[0] + grad_weight, running[1] + grad_bias, running[2] + grad_readout)
        return (running, (grad_values, partial_sums[0], partial_sums[1]))
    initial = (jnp.zeros_like(weights), jnp.zeros_like(biases), jnp.zeros_like(readout))
    summed, collected = lax.scan(per_block, initial, inputs)
    weight_sum, bias_sum, readout_sum = summed
    value_grads, residual_sums, misfit_sums = collected
    value_rows = value_grads.transpose(1, 0, 2).reshape(4, point_count)
    field_part = spread(flat_field.shape[0], cell_index, fractions, value_rows)
    energy, smooth_grad = smooth_field(conductivity, blocks)
    live_total = jnp.sum(live_count).astype(jnp.float32)
    conductivity_grad = field_part.reshape(conductivity.shape) + smooth_grad
    losses = jnp.stack([jnp.sum(residual_sums) / live_total, jnp.sum(misfit_sums) / live_total, energy / conductivity.size])
    return (conductivity_grad, weight_sum / live_total, bias_sum / live_total, readout_sum / live_total, losses)
```

```python
import functools

import jax
import jax.numpy as jnp
from jax import lax
from jax.experimental import pallas as pl
from jax.experimental.pallas import tpu as pltpu
from jax.sharding import PartitionSpec as P

TILE_SIDE = 32
LANES = 128
data_weight = 1.0
smooth_weight = 0.05
AXES = ("gx", "gy")
f32 = jnp.float32
bf16 = jnp.bfloat16
NN = (((1,), (0,)), ((), ()))
NT = (((1,), (1,)), ((), ()))


def dot(a, b, dims=NN):
    return lax.dot_general(a, b, dims, preferred_element_type=f32)


def split2(x):
    hi = x.astype(bf16)
    return hi, (x - hi.astype(f32)).astype(bf16)


def split3(x):
    hi = x.astype(bf16)
    rest = x - hi.astype(f32)
    mid = rest.astype(bf16)
    return hi, mid, (rest - mid.astype(f32)).astype(bf16)


def iota(shape, dim):
    return lax.broadcasted_iota(jnp.int32, shape, dim)


def sin_cos(phase):
    turns = jnp.floor(phase * 0.6366197723675814 + 0.5)
    y = phase - turns * 1.5703125
    y = y - turns * 4.837512969970703125e-4
    y = y - turns * 7.549789954891882e-8
    quarter = turns.astype(jnp.int32)
    y2 = y * y
    s = y + y * y2 * (-1.6666654611e-1 + y2 * (8.3321608736e-3 - y2 * 1.9515295891e-4))
    c = (
        1.0
        - 0.5 * y2
        + y2
        * y2
        * (4.166664568298827e-2 + y2 * (-1.388731625493765e-3 + y2 * 2.443315711809948e-5))
    )
    odd = (quarter & 1) == 1
    sin_part = jnp.where(odd, c, s)
    cos_part = jnp.where(odd, s, c)
    sin_part = jnp.where((quarter & 2) == 2, -sin_part, sin_part)
    cos_part = jnp.where(((quarter + 1) & 2) == 2, -cos_part, cos_part)
    return sin_part, cos_part


def activations(v, z1, z2, z3, z4):
    s = 1.0 - v * v
    q = z1 * z1 + z2 * z2 + z3 * z3
    return s, q, s * z4 - 2.0 * v * s * q


def slot_ranks_row(owner_col, owner_row):
    n = owner_row.shape[1]
    same = (owner_col == owner_row) & (iota((n, n), 0) < iota((n, n), 1))
    return jnp.sum(jnp.where(same, 1.0, 0.0), axis=0, keepdims=True).astype(jnp.int32)


def slot_ranks_col(owner_col, owner_row):
    n = owner_row.shape[1]
    same = (owner_col == owner_row) & (iota((n, n), 1) < iota((n, n), 0))
    return jnp.sum(jnp.where(same, 1.0, 0.0), axis=1, keepdims=True).astype(jnp.int32)


ROWS = 32


def forward_kernel(
    devices, layers, tiles,
    live_ref, owner_col_ref, owner_row_ref, slot_ref, offsets_ref, fractions_ref, source_ref,
    fourier_ref, weights_ref, small_ref,
    request_ref, pre_ref, first_ref, outputs_ref,
    hi_ref, lo_ref, z_ref, col_ref,
):
    points = slot_ref.shape[1]
    width = weights_ref.shape[1]
    streams = 5
    off = offsets_ref[...]
    fractions = fractions_ref[...]
    owner_row = owner_row_ref[...]
    slot = slot_ref[...]
    cells = jnp.concatenate(
        [TILE_SIDE * slot + off[0:1], TILE_SIDE * owner_row + off[1:2], off[2:3]], axis=0
    )
    position = cells.astype(f32) + fractions
    f = fourier_ref[...]
    phases = f[:, 0:1] * position[0:1] + f[:, 1:2] * position[1:2] + f[:, 2:3] * position[2:3]
    sin_part, cos_part = sin_cos(phases)
    squared = f[:, 0:1] * f[:, 0:1] + f[:, 1:2] * f[:, 1:2] + f[:, 2:3] * f[:, 2:3]
    freqs = f.shape[0]

    def put(stream, top, bottom):
        for start, value in ((0, top), (freqs, bottom)):
            rows = pl.ds(start, freqs)
            lanes = pl.ds(stream * points, points)
            first_ref[rows, lanes] = value
            hi, lo = split2(value)
            hi_ref[rows, lanes] = hi
            lo_ref[rows, lanes] = lo

    put(0, sin_part, cos_part)
    for k in range(3):
        put(k + 1, cos_part * f[:, k : k + 1], -sin_part * f[:, k : k + 1])
    put(4, -sin_part * squared, -cos_part * squared)

    small_cols = jnp.transpose(small_ref[...])
    readout_col = small_cols[:, layers : layers + 1]

    def layer(depth, sums):
        w_hi, w_lo = split2(weights_ref[depth])
        for k in range(streams):
            lanes = pl.ds(k * points, points)
            h_hi = hi_ref[:, lanes]
            z_ref[:, lanes] = dot(w_hi, h_hi) + dot(w_hi, lo_ref[:, lanes]) + dot(w_lo, h_hi)
        bias = jnp.sum(
            jnp.where(iota(small_cols.shape, 1) == depth, small_cols, 0.0), axis=1, keepdims=True
        )
        col_ref[:, 0:1] = bias
        col_ref[:, 1:2] = readout_col

        def chunk(c, totals):
            rows = pl.ds(pl.multiple_of(c * ROWS, ROWS), ROWS)

            def z_of(k):
                return z_ref[rows, pl.ds(k * points, points)]

            v = jnp.tanh(z_of(0) + col_ref[rows, 0:1])
            z1, z2, z3, z4 = z_of(1), z_of(2), z_of(3), z_of(4)
            s, _, curve = activations(v, z1, z2, z3, z4)
            r = col_ref[rows, 1:2]
            new = []
            for k, (kept, h) in enumerate(
                ((v, v), (z1, s * z1), (z2, s * z2), (z3, s * z3), (z4, curve))
            ):
                lanes = pl.ds(k * points, points)
                pre_ref[depth, rows, lanes] = kept
                hi, lo = split2(h)
                hi_ref[rows, lanes] = hi
                lo_ref[rows, lanes] = lo
                new.append(totals[k] + jnp.sum(r * h, axis=0, keepdims=True))
            return tuple(new)

        zero = tuple(jnp.zeros((1, points), f32) for _ in range(streams))
        return lax.fori_loop(0, width // ROWS, chunk, zero)

    zero = tuple(jnp.zeros((1, points), f32) for _ in range(streams))
    out = lax.fori_loop(0, layers, layer, zero)
    outputs = jnp.concatenate(list(out) + [jnp.zeros((3, points), f32)], axis=0)
    outputs_ref[...] = outputs

    live = jnp.where(iota((1, points), 1) < live_ref[0, 0], 1.0, 0.0)
    row_index = ((off[0:1] * (TILE_SIDE // 4) + off[1:2] // 4) * tiles + slot).astype(f32)
    lane_index = ((off[1:2] % 4) * TILE_SIDE + off[2:3]).astype(f32)
    comps = [
        row_index, lane_index, fractions[0:1], fractions[1:2], fractions[2:3],
        outputs[1:2], outputs[2:3], outputs[3:4], outputs[4:5], source_ref[...], live,
    ]
    to_owner = owner_row == iota((devices, points), 0)
    ranks = slot_ranks_col(owner_col_ref[...], owner_row)
    place = jnp.where(ranks == iota((points, LANES), 1), 1.0, 0.0).astype(bf16)
    spread = jnp.concatenate([jnp.where(to_owner, c, 0.0) for c in comps], axis=0)
    a, b, c = split3(spread)
    packed = dot(a, place) + dot(b, place) + dot(c, place)
    for k in range(len(comps)):
        request_ref[:, k, :] = packed[k * devices : (k + 1) * devices]
    for k in range(len(comps), request_ref.shape[1]):
        request_ref[:, k, :] = jnp.zeros((devices, LANES), f32)


def owner_kernel(
    devices, tiles, lanes_each,
    received_ref, field_ref,
    response_ref, kept_ref,
    padded_ref, window_hi, window_lo, x_ref,
):
    cells = field_ref.shape[0]
    group = LANES // lanes_each
    blocks = devices // group
    slots = blocks * LANES
    plane = (TILE_SIDE // 4) * tiles
    padded_ref[0:cells, :] = field_ref[...]
    padded_ref[cells:, :] = jnp.zeros((padded_ref.shape[0] - cells, LANES), f32)
    for a in range(2):
        base = a * plane
        main = jnp.transpose(padded_ref[base : base + cells, :])
        hi, lo = split2(main)
        window_hi[a * 160 : a * 160 + 128, :] = hi
        window_lo[a * 160 : a * 160 + 128, :] = lo
        extra = jnp.transpose(padded_ref[base + tiles : base + tiles + cells, :])[0:TILE_SIDE]
        hi, lo = split2(extra)
        window_hi[a * 160 + 128 : a * 160 + 160, :] = hi
        window_lo[a * 160 + 128 : a * 160 + 160, :] = lo
    for j in range(blocks):
        total = received_ref[group * j]
        for m in range(1, group):
            total = total + pltpu.roll(received_ref[group * j + m], lanes_each * m, 1)
        x_ref[:, j * LANES : (j + 1) * LANES] = total

    step = 2 * LANES
    for start in range(0, slots, step):
        x = x_ref[:, start : start + step]
        rows = x[0:1].astype(jnp.int32)
        place = x[1:2].astype(jnp.int32)
        hot = jnp.where(iota((cells, step), 0) == rows, 1.0, 0.0).astype(bf16)
        found = dot(window_hi[...], hot) + dot(window_lo[...], hot)
        y_mod = place // TILE_SIDE
        z_cell = place % TILE_SIDE
        z_iota = iota((TILE_SIDE, step), 0)
        at_z = (z_iota == z_cell, z_iota == z_cell + 1)
        corner = {}
        for a in range(2):
            parts = [found[a * 160 + TILE_SIDE * j : a * 160 + TILE_SIDE * (j + 1)] for j in range(5)]
            for b in range(2):
                rows_y = jnp.where(y_mod == 0, parts[b], 0.0)
                for j in range(1, 4):
                    rows_y = jnp.where(y_mod == j, parts[j + b], rows_y)
                for c in range(2):
                    corner[a, b, c] = jnp.sum(
                        jnp.where(at_z[c], rows_y, 0.0), axis=0, keepdims=True
                    )
        fr = [x[2:3], x[3:4], x[4:5]]
        w = [(1.0 - t, t) for t in fr]
        sign = (-1.0, 1.0)
        values = [jnp.zeros((1, step), f32) for _ in range(4)]
        for (a, b, c), k in corner.items():
            values[0] = values[0] + w[0][a] * w[1][b] * w[2][c] * k
            values[1] = values[1] + sign[a] * w[1][b] * w[2][c] * k
            values[2] = values[2] + w[0][a] * sign[b] * w[2][c] * k
            values[3] = values[3] + w[0][a] * w[1][b] * sign[c] * k
        du = [x[5:6], x[6:7], x[7:8]]
        lap = x[8:9]
        residual = (
            -(values[0] * lap + (values[1] * du[0] + values[2] * du[1] + values[3] * du[2]))
            - x[9:10]
        )
        scaled = 2.0 * x[10:11] * residual
        zeros = jnp.zeros((4, step), f32)
        answer = jnp.concatenate(values + [zeros], axis=0)
        for j in range(step // LANES):
            block = start // LANES + j
            part = answer[:, j * LANES : (j + 1) * LANES]
            for m in range(group):
                shifted = pltpu.roll(part, (LANES - lanes_each * m) % LANES, 1) if m else part
                response_ref[group * block + m] = shifted
        kept_ref[:, start : start + step] = jnp.concatenate(
            [x[0:5], -scaled * lap, -scaled * du[0], -scaled * du[1], -scaled * du[2]]
            + [jnp.zeros((7, step), f32)],
            axis=0,
        )


def field_kernel(
    devices, tiles,
    index_ref, kept_ref, field_ref, before_ref, after_ref,
    grad_ref, energy_ref,
    hot_ref, c_hi, c_lo, sum_ref, part_ref,
):
    cells = field_ref.shape[0]
    slots = kept_ref.shape[1]
    plane = (TILE_SIDE // 4) * tiles
    step = 2 * LANES
    for start in range(0, slots, step):
        lanes = slice(start, start + step)
        x = kept_ref[:, lanes]
        rows = x[0:1].astype(jnp.int32)
        place = x[1:2].astype(jnp.int32)
        hot_ref[:, lanes] = jnp.where(iota((cells, step), 0) == rows, 1.0, 0.0).astype(bf16)
        y_mod = place // TILE_SIDE
        z_cell = place % TILE_SIDE
        z_iota = iota((TILE_SIDE, step), 0)
        at_z = (z_iota == z_cell, z_iota == z_cell + 1)
        w = [(1.0 - x[k : k + 1], x[k : k + 1]) for k in (2, 3, 4)]
        g = [x[k : k + 1] for k in (5, 6, 7, 8)]
        sign = (-1.0, 1.0)
        for a in range(2):
            along = []
            for b in range(2):
                pair = []
                for c in range(2):
                    pair.append(
                        g[0] * w[0][a] * w[1][b] * w[2][c]
                        + g[1] * sign[a] * w[1][b] * w[2][c]
                        + g[2] * w[0][a] * sign[b] * w[2][c]
                        + g[3] * w[0][a] * w[1][b] * sign[c]
                    )
                along.append(jnp.where(at_z[0], pair[0], 0.0) + jnp.where(at_z[1], pair[1], 0.0))
            for j in range(5):
                value = jnp.where(y_mod == j, along[0], 0.0) + jnp.where(
                    y_mod == j - 1, along[1], 0.0
                )
                hi, lo = split2(value)
                at = a * 128 + TILE_SIDE * j if j < 4 else 256 + a * TILE_SIDE
                c_hi[at : at + TILE_SIDE, lanes] = hi
                c_lo[at : at + TILE_SIDE, lanes] = lo
    sum_ref[...] = jnp.zeros(sum_ref.shape, f32)
    block = 2 * LANES
    for start in range(0, cells, block):
        hot = hot_ref[start : start + block, :]
        part = dot(hot, c_hi[...], NT) + dot(hot, c_lo[...], NT)
        part_ref[start : start + block, :] = part
    sum_ref[0:cells, :] = part_ref[:, 0:128]
    sum_ref[plane : plane + cells, :] += part_ref[:, 128:256]
    low = slice(0, TILE_SIDE)
    sum_ref[tiles : tiles + cells, low] += part_ref[:, 256 : 256 + TILE_SIDE]
    sum_ref[plane + tiles : plane + tiles + cells, low] += part_ref[
        :, 256 + TILE_SIDE : 256 + 2 * TILE_SIDE
    ]

    me = index_ref[0, 0]
    row = iota((plane, LANES), 0)
    lane = iota((plane, LANES), 1)
    z_inner = (lane % TILE_SIDE) < TILE_SIDE - 1
    first_row = row < tiles
    last_row = row >= plane - tiles
    low_lane = lane < TILE_SIDE
    high_lane = lane >= LANES - TILE_SIDE
    has_after = jnp.where(me < devices - 1, 1.0, 0.0)
    has_before = jnp.where(me > 0, 1.0, 0.0)
    after_mask = jnp.where(last_row & high_lane, has_after, 1.0)
    before_mask = jnp.where(first_row & low_lane, has_before, 1.0)
    energy_mask = before_mask
    next_tile = (row % tiles) < tiles - 1
    prev_tile = (row % tiles) > 0

    def load(x):
        return field_ref[pl.ds(pl.multiple_of(x * plane, plane), plane), :]

    def plane_step(x, energy):
        here = load(x)
        diff_z = jnp.where(z_inner, pltpu.roll(here, LANES - 1, 1) - here, 0.0)
        grad = pltpu.roll(diff_z, 1, 1) - diff_z
        energy = energy + diff_z * diff_z
        above = jnp.concatenate([here[tiles:], after_ref[x]], axis=0)
        up = pltpu.roll(jnp.where(low_lane, above, here), LANES - TILE_SIDE, 1)
        below = jnp.concatenate([before_ref[x], here[: plane - tiles]], axis=0)
        down = pltpu.roll(jnp.where(high_lane, below, here), TILE_SIDE, 1)
        diff_up = (up - here) * after_mask
        diff_down = (here - down) * before_mask
        grad = grad + diff_down - diff_up
        energy = energy + diff_down * diff_down
        first = x == 0
        last = x == TILE_SIDE - 1
        nxt = load(jnp.where(last, 0, x + 1))
        nxt = jnp.where(last, pltpu.roll(nxt, plane - 1, 0), nxt)
        prv = load(jnp.where(first, TILE_SIDE - 1, x - 1))
        prv = jnp.where(first, pltpu.roll(prv, 1, 0), prv)
        diff_next = jnp.where(jnp.logical_not(last) | next_tile, nxt - here, 0.0)
        diff_prev = jnp.where(jnp.logical_not(first) | prev_tile, here - prv, 0.0)
        grad = grad + diff_prev - diff_next
        energy = energy + diff_prev * diff_prev
        at = pl.ds(pl.multiple_of(x * plane, plane), plane)
        grad_ref[at, :] = sum_ref[at, :] + 2.0 * smooth_weight * grad
        return energy

    energy = lax.fori_loop(0, TILE_SIDE, plane_step, jnp.zeros((plane, LANES), f32))
    total = jnp.sum(energy, axis=0, keepdims=True)
    wide = jnp.concatenate([total, jnp.zeros((1, energy_ref.shape[1] - LANES), f32)], axis=1)
    energy_ref[...] = jnp.where(iota(energy_ref.shape, 0) == 0, wide, 0.0)


def backward_kernel(
    devices, layers, lanes_each,
    scalars_ref, owner_col_ref, owner_row_ref, source_ref, observed_ref, response_ref,
    outputs_ref, weights_ref, small_ref, pre_ref, first_ref,
    keep_ref, send_ref,
    bar_ref, zh_ref, zl_ref, hh_ref, hl_ref, col_ref, cols_ref,
):
    points = owner_row_ref.shape[1]
    width = weights_ref.shape[1]
    owner_row = owner_row_ref[...]
    ranks = slot_ranks_row(owner_col_ref[...], owner_row)
    picked = jnp.where(ranks == iota((lanes_each, points), 0), 1.0, 0.0)
    from_owner = jnp.where(owner_row == iota((devices, points), 0), 1.0, 0.0).astype(bf16)
    values = []
    for k in range(4):
        rows = jnp.transpose(response_ref[:, k, :])[0:lanes_each]
        a, b, c = split3(rows)
        wide = dot(a, from_owner) + dot(b, from_owner) + dot(c, from_owner)
        values.append(jnp.sum(picked * wide, axis=0, keepdims=True))
    outputs = outputs_ref[...]
    out = [outputs[k : k + 1] for k in range(5)]
    live = jnp.where(iota((1, points), 1) < scalars_ref[0, 0], 1.0, 0.0)
    misfit = out[0] - observed_ref[...]
    residual = (
        -(values[0] * out[4] + (values[1] * out[1] + values[2] * out[2] + values[3] * out[3]))
        - source_ref[...]
    )
    scaled = 2.0 * live * residual
    out_grad = [2.0 * data_weight * live * misfit] + [-scaled * values[k] for k in (1, 2, 3, 0)]
    residual_sum = jnp.sum(live * residual * residual, axis=1, keepdims=True)
    misfit_sum = jnp.sum(live * misfit * misfit, axis=1, keepdims=True)
    small_cols = jnp.transpose(small_ref[...])
    readout_col = small_cols[:, layers : layers + 1]
    col_ref[...] = readout_col
    cols_ref[...] = jnp.zeros(cols_ref.shape, f32)
    lane8 = iota((ROWS, cols_ref.shape[1]), 1)
    chunks = width // ROWS

    def rows_of(c):
        return pl.ds(pl.multiple_of(c * ROWS, ROWS), ROWS)

    def pre_of(depth, rows):
        return [pre_ref[depth, rows, pl.ds(k * points, points)] for k in range(5)]

    def readout_chunk(c, carry):
        rows = rows_of(c)
        v, z1, z2, z3, z4 = pre_of(layers - 1, rows)
        s, _, curve = activations(v, z1, z2, z3, z4)
        total = out_grad[0] * v + out_grad[1] * (s * z1) + out_grad[2] * (s * z2)
        total = total + out_grad[3] * (s * z3) + out_grad[4] * curve
        grad = jnp.sum(total, axis=1, keepdims=True)
        cols_ref[rows, :] += jnp.where(lane8 == layers, grad, 0.0)
        r = col_ref[rows, :]
        for k in range(5):
            bar_ref[rows, pl.ds(k * points, points)] = r * out_grad[k]
        return carry

    lax.fori_loop(0, chunks, readout_chunk, 0)
    mine = scalars_ref[0, 1]
    half = layers // 2

    def layer(step, carry):
        depth = layers - 1 - step

        def bars(c, inner):
            rows = rows_of(c)
            v, z1, z2, z3, z4 = pre_of(depth, rows)
            b = [bar_ref[rows, pl.ds(k * points, points)] for k in range(5)]
            s = 1.0 - v * v
            q = z1 * z1 + z2 * z2 + z3 * z3
            slope = b[1] * z1 + b[2] * z2 + b[3] * z3
            v4c = 4.0 * v * b[4]
            z_bar = [
                s
                * (
                    b[0]
                    - 2.0 * v * slope
                    + b[4] * (q * (4.0 * v * v - 2.0 * s) - 2.0 * v * z4)
                ),
                s * (b[1] - v4c * z1),
                s * (b[2] - v4c * z2),
                s * (b[3] - v4c * z3),
                s * b[4],
            ]
            grad = jnp.sum(z_bar[0], axis=1, keepdims=True)
            cols_ref[rows, :] += jnp.where(lane8 == depth, grad, 0.0)
            for k in range(5):
                lanes = pl.ds(k * points, points)
                hi, lo = split2(z_bar[k])
                zh_ref[rows, lanes] = hi
                zl_ref[rows, lanes] = lo
            return inner

        lax.fori_loop(0, chunks, bars, 0)

        def put_h(rows, hs):
            for k in range(5):
                lanes = pl.ds(k * points, points)
                hi, lo = split2(hs[k])
                hh_ref[rows, lanes] = hi
                hl_ref[rows, lanes] = lo

        @pl.when(depth > 0)
        def _():
            def body(c, inner):
                rows = rows_of(c)
                v, z1, z2, z3, z4 = pre_of(jnp.maximum(depth - 1, 0), rows)
                s, _, curve = activations(v, z1, z2, z3, z4)
                put_h(rows, [v, s * z1, s * z2, s * z3, curve])
                return inner

            lax.fori_loop(0, chunks, body, 0)

        @pl.when(depth == 0)
        def _():
            def body(c, inner):
                rows = rows_of(c)
                put_h(rows, [first_ref[rows, pl.ds(k * points, points)] for k in range(5)])
                return inner

            lax.fori_loop(0, chunks, body, 0)

        grad = (
            dot(zh_ref[...], hh_ref[...], NT)
            + dot(zh_ref[...], hl_ref[...], NT)
            + dot(zl_ref[...], hh_ref[...], NT)
        )
        upper = (depth >= half).astype(jnp.int32)
        at = pl.ds(pl.multiple_of((depth - upper * half) * width, width), width)

        @pl.when(upper == mine)
        def _():
            keep_ref[at, :] = grad

        @pl.when(upper != mine)
        def _():
            send_ref[at, :] = grad

        @pl.when(depth > 0)
        def _():
            w_hi, w_lo = split2(jnp.transpose(weights_ref[depth]))
            for k in range(5):
                lanes = pl.ds(k * points, points)
                z_hi = zh_ref[:, lanes]
                bar_ref[:, lanes] = dot(w_hi, z_hi) + dot(w_hi, zl_ref[:, lanes]) + dot(w_lo, z_hi)

        return carry

    lax.fori_loop(0, layers, layer, 0)
    small = jnp.transpose(cols_ref[...])
    lane = iota((1, width), 1)
    count = jnp.full((1, 1), scalars_ref[0, 0], jnp.int32).astype(f32)
    last = jnp.where(lane == 0, residual_sum, 0.0) + jnp.where(lane == 1, misfit_sum, 0.0)
    last = last + jnp.where(lane == 2, count, 0.0)
    small = jnp.where(iota(small.shape, 0) == small.shape[0] - 1, last, small)
    keep_ref[half * width :, :] = small
    send_ref[half * width :, :] = small


def vmem():
    return pl.BlockSpec(memory_space=pltpu.VMEM)


def smem():
    return pl.BlockSpec(memory_space=pltpu.SMEM)


def call(kernel, name, specs, out_shapes, scratch, flops, limit=40):
    return pl.pallas_call(
        kernel,
        name=name,
        out_shape=out_shapes,
        in_specs=specs,
        out_specs=jax.tree.map(lambda _: vmem(), out_shapes),
        scratch_shapes=scratch,
        compiler_params=pltpu.CompilerParams(vmem_limit_bytes=limit << 20),
        cost_estimate=pl.CostEstimate(flops=flops, bytes_accessed=1 << 20, transcendentals=0),
    )


def shape(*dims):
    return jax.ShapeDtypeStruct(dims, f32)


def on_device(
    conductivity, owner_rank, tile_slot, offsets, fractions, source, observed, live_count,
    fourier, weights, biases, readout,
):
    devices = lax.axis_size(AXES)
    index = lax.axis_index(AXES)
    points = tile_slot.shape[0]
    tiles = conductivity.shape[0]
    layers, width = biases.shape
    capacity = (2 * points + devices - 1) // devices + 1
    lanes_each = 1 << (capacity - 1).bit_length()
    lanes_each = max(lanes_each, 2 * LANES // devices)
    slots = devices * lanes_each
    cells = conductivity.size // LANES
    plane = (TILE_SIDE // 4) * tiles
    wide = 5 * points

    owner_row = owner_rank.reshape(1, points)
    slot = tile_slot.reshape(1, points)
    source_row = source.reshape(1, points)
    observed_row = observed.reshape(1, points)
    small = jnp.concatenate(
        [biases, readout[None], jnp.zeros((8 - layers - 1, width), f32)], axis=0
    )
    field = conductivity.reshape(tiles, cells // tiles, LANES).transpose(1, 0, 2)
    field = field.reshape(cells, LANES)
    planes = field.reshape(TILE_SIDE, plane, LANES)

    request, pre, first, outputs = call(
        functools.partial(forward_kernel, devices, layers, tiles),
        "forward",
        [smem()] + [vmem()] * 9,
        (shape(devices, 16, LANES), shape(layers, width, wide), shape(width, wide), shape(8, points)),
        [
            pltpu.VMEM((width, wide), bf16),
            pltpu.VMEM((width, wide), bf16),
            pltpu.VMEM((width, wide), f32),
            pltpu.VMEM((width, 2), f32),
        ],
        6 * 2 * layers * width * width * wide,
    )(
        live_count.reshape(1, 1), owner_rank, owner_row, slot, offsets, fractions, source_row,
        fourier, weights, small,
    )
    received = lax.all_to_all(request, AXES, split_axis=0, concat_axis=0, tiled=True)
    response, kept = call(
        functools.partial(owner_kernel, devices, tiles, lanes_each),
        "lookup",
        [vmem()] * 2,
        (shape(devices, 8, LANES), shape(16, slots)),
        [
            pltpu.VMEM((cells + 2 * plane, LANES), f32),
            pltpu.VMEM((320, cells), bf16),
            pltpu.VMEM((320, cells), bf16),
            pltpu.VMEM((16, slots), f32),
        ],
        2 * 640 * cells * slots,
    )(received, field)
    answered = lax.all_to_all(response, AXES, split_axis=0, concat_axis=0, tiled=True)

    up = [(i, i + 1) for i in range(devices - 1)]
    down = [(j, i) for i, j in up]
    before = lax.ppermute(planes[:, plane - tiles :, :], AXES, up)
    after = lax.ppermute(planes[:, :tiles, :], AXES, down)

    half_rows = layers * width // 2
    core = index % 2
    scalars = jnp.stack([live_count[0], core]).reshape(1, 2)
    keep, send = call(
        functools.partial(backward_kernel, devices, layers, lanes_each),
        "backward",
        [smem()] + [vmem()] * 10,
        (shape(half_rows + 8, width), shape(half_rows + 8, width)),
        [
            pltpu.VMEM((width, wide), f32),
            pltpu.VMEM((width, wide), bf16),
            pltpu.VMEM((width, wide), bf16),
            pltpu.VMEM((width, wide), bf16),
            pltpu.VMEM((width, wide), bf16),
            pltpu.VMEM((width, 1), f32),
            pltpu.VMEM((width, 8), f32),
        ],
        12 * 2 * layers * width * width * wide,
    )(
        scalars, owner_rank, owner_row, source_row, observed_row, answered, outputs, weights,
        small, pre, first,
    )
    grad, energy = call(
        functools.partial(field_kernel, devices, tiles),
        "field",
        [smem()] + [vmem()] * 4,
        (shape(cells, LANES), shape(8, width)),
        [
            pltpu.VMEM((cells, slots), bf16),
            pltpu.VMEM((320, slots), bf16),
            pltpu.VMEM((320, slots), bf16),
            pltpu.VMEM((cells + 2 * plane, LANES), f32),
            pltpu.VMEM((cells, 320), f32),
        ],
        2 * 640 * cells * slots,
    )(index.reshape(1, 1), kept, field, before, after)

    bits = [1 << k for k in range(devices.bit_length() - 1)]

    def exchange(value, bit):
        return lax.ppermute(value, AXES, [(i, i ^ bit) for i in range(devices)])

    arrived = exchange(send, bits[0])
    current = keep + arrived
    main, extra = current[:half_rows], current[half_rows:]
    for bit in bits[1:]:
        half = main.shape[0] // 2
        upper = (index // bit) % 2 == 1
        low, high = main[:half], main[half:]
        outgoing = jnp.concatenate([jnp.where(upper, low, high), extra], axis=0)
        arrived = exchange(outgoing, bit)
        main = jnp.where(upper, high, low) + arrived[:half]
        extra = extra + arrived[half:]
    live_total = extra[7, 2]
    main = main / live_total
    for bit in reversed(bits):
        upper = (index // bit) % 2 == 1
        arrived = exchange(jnp.concatenate([main, energy], axis=0), bit)
        other = arrived[: main.shape[0]]
        energy = energy + arrived[main.shape[0] :]
        main = jnp.concatenate(
            [jnp.where(upper, other, main), jnp.where(upper, main, other)], axis=0
        )
    cells_total = devices * conductivity.size
    losses = jnp.stack(
        [extra[7, 0] / live_total, extra[7, 1] / live_total, jnp.sum(energy) / cells_total]
    )
    conductivity_grad = grad.reshape(cells // tiles, tiles, LANES).transpose(1, 0, 2)
    return (
        conductivity_grad.reshape(conductivity.shape),
        main.reshape(weights.shape),
        extra[:layers] / live_total,
        extra[layers] / live_total,
        losses,
    )


def solution(mesh):
    in_specs = (
        P(AXES, None), P(AXES, None), P(AXES), P(None, AXES), P(None, AXES), P(AXES), P(AXES),
        P(AXES), P(), P(), P(), P(),
    )
    out_specs = (P(AXES, None), P(), P(), P(), P())
    return jax.shard_map(
        on_device, mesh=mesh, in_specs=in_specs, out_specs=out_specs, check_vma=False
    )
```

```python
import functools

import jax
import jax.numpy as jnp
from jax import lax
from jax.experimental import pallas as pl
from jax.experimental.pallas import tpu as pltpu
from jax.sharding import PartitionSpec as P

TILE_SIDE = 32
LANES = 128
data_weight = 1.0
smooth_weight = 0.05
AXES = ("gx", "gy")
f32 = jnp.float32
bf16 = jnp.bfloat16
NN = (((1,), (0,)), ((), ()))
NT = (((1,), (1,)), ((), ()))


def dot(a, b, dims=NN):
    return lax.dot_general(a, b, dims, preferred_element_type=f32)


def split2(x):
    hi = x.astype(bf16)
    return hi, (x - hi.astype(f32)).astype(bf16)


def split3(x):
    hi = x.astype(bf16)
    rest = x - hi.astype(f32)
    mid = rest.astype(bf16)
    return hi, mid, (rest - mid.astype(f32)).astype(bf16)


def iota(shape, dim):
    return lax.broadcasted_iota(jnp.int32, shape, dim)


def sin_cos(phase):
    turns = jnp.floor(phase * 0.6366197723675814 + 0.5)
    y = phase - turns * 1.5703125
    y = y - turns * 4.837512969970703125e-4
    y = y - turns * 7.549789954891882e-8
    quarter = turns.astype(jnp.int32)
    y2 = y * y
    s = y + y * y2 * (-1.6666654611e-1 + y2 * (8.3321608736e-3 - y2 * 1.9515295891e-4))
    c = (
        1.0
        - 0.5 * y2
        + y2
        * y2
        * (4.166664568298827e-2 + y2 * (-1.388731625493765e-3 + y2 * 2.443315711809948e-5))
    )
    odd = (quarter & 1) == 1
    sin_part = jnp.where(odd, c, s)
    cos_part = jnp.where(odd, s, c)
    sin_part = jnp.where((quarter & 2) == 2, -sin_part, sin_part)
    cos_part = jnp.where(((quarter + 1) & 2) == 2, -cos_part, cos_part)
    return sin_part, cos_part


def activations(v, z1, z2, z3, z4):
    s = 1.0 - v * v
    q = z1 * z1 + z2 * z2 + z3 * z3
    return s, q, s * z4 - 2.0 * v * s * q


def column_of(row):
    wide = jnp.broadcast_to(row.astype(f32), (8, row.shape[1]))
    return jnp.transpose(wide)[:, 0:1].astype(row.dtype)


def slot_ranks_row(owner_col, owner_row):
    n = owner_row.shape[1]
    same = (owner_col == owner_row) & (iota((n, n), 0) < iota((n, n), 1))
    return jnp.sum(jnp.where(same, 1.0, 0.0), axis=0, keepdims=True).astype(jnp.int32)


def slot_ranks_col(owner_col, owner_row):
    n = owner_row.shape[1]
    same = (owner_col == owner_row) & (iota((n, n), 1) < iota((n, n), 0))
    return jnp.sum(jnp.where(same, 1.0, 0.0), axis=1, keepdims=True).astype(jnp.int32)


ROWS = 32
FILL = 4 * 10**9
FORWARD_LIMIT, PREPARE_LIMIT, LOOKUP_LIMIT, SPREAD_LIMIT, BACKWARD_LIMIT = 64, 8, 12, 14, 58


def forward_kernel(
    devices, layers, tiles, lanes_each,
    live_ref, owner_hbm, slot_hbm, offsets_hbm, fractions_hbm, source_hbm,
    fourier_hbm, weights_hbm, biases_hbm, readout_hbm,
    request_ref, outputs_ref, pre_hbm, parts_hbm,
    pre_ref, parts_ref, weights_ref, z_ref, col_ref, bias_ref,
    owner_ref, slot_ref, offsets_ref, fractions_ref, source_ref, fourier_ref, small_ref,
    freq_ref, biases_ref, readout_ref, sems, out_sems,
):
    small_ref[...] = jnp.zeros(small_ref.shape, f32)
    fourier_ref[...] = jnp.zeros(fourier_ref.shape, f32)
    copies = [
        pltpu.make_async_copy(source, target, sems.at[k])
        for k, (source, target) in enumerate(
            (
                (owner_hbm, owner_ref), (slot_hbm, slot_ref), (offsets_hbm, offsets_ref),
                (fractions_hbm, fractions_ref), (fourier_hbm, freq_ref),
                (source_hbm, source_ref), (biases_hbm, biases_ref),
                (readout_hbm, readout_ref), (weights_hbm, weights_ref),
            )
        )
    ]
    for copy in copies:
        copy.start()
    for copy in copies[:-1]:
        copy.wait()
    fourier_ref[0:3, :] = freq_ref[...]
    small_ref[0:layers, :] = biases_ref[...]
    small_ref[layers : layers + 1, :] = readout_ref[...]
    points = slot_ref.shape[1]
    width = weights_ref.shape[1]
    streams = 5
    off = offsets_ref[...]
    fractions = fractions_ref[...]
    owner_row = owner_ref[...]
    slot = slot_ref[...]
    cells = jnp.concatenate(
        [TILE_SIDE * slot + off[0:1], TILE_SIDE * owner_row + off[1:2], off[2:3]], axis=0
    )
    position = cells.astype(f32) + fractions
    f = jnp.transpose(fourier_ref[...])
    phases = f[:, 0:1] * position[0:1] + f[:, 1:2] * position[1:2] + f[:, 2:3] * position[2:3]
    sin_part, cos_part = sin_cos(phases)
    squared = f[:, 0:1] * f[:, 0:1] + f[:, 1:2] * f[:, 1:2] + f[:, 2:3] * f[:, 2:3]
    freqs = f.shape[0]

    def put(stream, top, bottom):
        for start, value in ((0, top), (freqs, bottom)):
            lanes = pl.ds(stream * points, points)
            hi, lo = split2(value)
            parts_ref[0, pl.ds(start, freqs), lanes] = hi
            parts_ref[0, pl.ds(width + start, freqs), lanes] = lo

    put(0, sin_part, cos_part)
    for k in range(3):
        put(k + 1, cos_part * f[:, k : k + 1], -sin_part * f[:, k : k + 1])
    put(4, -sin_part * squared, -cos_part * squared)

    small_cols = jnp.transpose(small_ref[...])
    col_ref[...] = small_cols
    copies[-1].wait()

    def leave_parts(depth):
        return pltpu.make_async_copy(
            parts_ref.at[depth], parts_hbm.at[depth], out_sems.at[0, depth]
        )

    def leave_pre(depth):
        return pltpu.make_async_copy(pre_ref.at[depth], pre_hbm.at[depth], out_sems.at[1, depth])

    def layer(depth, carry):
        leave_parts(depth).start()
        w_hi, w_lo = split2(weights_ref[depth])
        for k in range(streams):
            lanes = pl.ds(k * points, points)
            h_hi = parts_ref[depth, 0:width, lanes]
            h_lo = parts_ref[depth, width:, lanes]
            z_ref[:, lanes] = dot(w_hi, h_hi) + dot(w_hi, h_lo) + dot(w_lo, h_hi)
        bias = jnp.sum(
            jnp.where(iota(small_cols.shape, 1) == depth, small_cols, 0.0), axis=1, keepdims=True
        )
        bias_ref[...] = bias

        def chunk(c, inner):
            rows = pl.ds(pl.multiple_of(c * ROWS, ROWS), ROWS)
            low_rows = pl.ds(pl.multiple_of(width + c * ROWS, ROWS), ROWS)

            def z_of(k):
                return z_ref[rows, pl.ds(k * points, points)]

            v = jnp.tanh(z_of(0) + bias_ref[rows, :])
            z1, z2, z3, z4 = z_of(1), z_of(2), z_of(3), z_of(4)
            s, _, curve = activations(v, z1, z2, z3, z4)
            for k, (kept, h) in enumerate(
                ((v, v), (z1, s * z1), (z2, s * z2), (z3, s * z3), (z4, curve))
            ):
                lanes = pl.ds(k * points, points)
                pre_ref[depth, rows, lanes] = kept
                hi, lo = split2(h)
                parts_ref[depth + 1, rows, lanes] = hi
                parts_ref[depth + 1, low_rows, lanes] = lo
            return inner

        lax.fori_loop(0, width // ROWS, chunk, 0)
        leave_pre(depth).start()
        return carry

    lax.fori_loop(0, layers, layer, 0)

    def readout_chunk(c, totals):
        rows = pl.ds(pl.multiple_of(c * ROWS, ROWS), ROWS)
        v, z1, z2, z3, z4 = [
            pre_ref[layers - 1, rows, pl.ds(k * points, points)] for k in range(streams)
        ]
        s, _, curve = activations(v, z1, z2, z3, z4)
        r = col_ref[rows, layers : layers + 1]
        hs = (v, s * z1, s * z2, s * z3, curve)
        return tuple(t + jnp.sum(r * h, axis=0, keepdims=True) for t, h in zip(totals, hs))

    zero = tuple(jnp.zeros((1, points), f32) for _ in range(streams))
    out = lax.fori_loop(0, width // ROWS, readout_chunk, zero)
    outputs = jnp.concatenate(list(out) + [jnp.zeros((3, points), f32)], axis=0)
    outputs_ref[...] = outputs

    live = jnp.where(iota((1, points), 1) < live_ref[0, 0], 1.0, 0.0)
    row_index = ((off[0:1] * (TILE_SIDE // 4) + off[1:2] // 4) * tiles + slot).astype(f32)
    lane_index = ((off[1:2] % 4) * TILE_SIDE + off[2:3]).astype(f32)
    comps = [
        row_index, lane_index, fractions[0:1], fractions[1:2], fractions[2:3],
        outputs[1:2], outputs[2:3], outputs[3:4], outputs[4:5], source_ref[...], live,
    ]
    to_owner = owner_row == iota((devices, points), 0)
    ranks = slot_ranks_col(column_of(owner_row), owner_row)
    place = jnp.where(ranks == iota((points, LANES), 1), 1.0, 0.0).astype(bf16)
    spread = jnp.concatenate([jnp.where(to_owner, c, 0.0) for c in comps], axis=0)
    a, b, c = split3(spread)
    packed = dot(a, place) + dot(b, place) + dot(c, place)
    rows_each, lane_groups = request_ref.shape[1], LANES // lanes_each
    for j in range(rows_each):
        total = jnp.zeros((devices, LANES), f32)
        for m in range(lane_groups):
            k = rows_each * m + j
            if k < len(comps):
                part = packed[k * devices : (k + 1) * devices]
                total = total + (pltpu.roll(part, lanes_each * m, 1) if m else part)
        request_ref[:, j, :] = total
    for depth in range(layers):
        leave_parts(depth).wait()
        leave_pre(depth).wait()


def owner_kernel(
    devices, tiles, lanes_each,
    received_ref, window_hi, window_lo,
    response_ref, kept_ref,
    x_ref,
):
    cells = window_hi.shape[1]
    group = LANES // lanes_each
    blocks = devices // group
    slots = blocks * LANES
    rows_each = received_ref.shape[1]
    lane_block = iota((rows_each * group, LANES), 1) // lanes_each
    for j in range(blocks):
        total = None
        for g in range(group):
            part = received_ref[group * j + g]
            moved = jnp.concatenate(
                [
                    pltpu.roll(part, lanes_each * ((g - m) % group), 1) if g != m else part
                    for m in range(group)
                ],
                axis=0,
            )
            total = moved if total is None else jnp.where(lane_block == g, moved, total)
        x_ref[:, j * LANES : (j + 1) * LANES] = total

    step = 2 * LANES
    for start in range(0, slots, step):
        x = x_ref[:, start : start + step]
        rows = x[0:1].astype(jnp.int32)
        place = x[1:2].astype(jnp.int32)
        hot = jnp.where(iota((cells, step), 0) == rows, 1.0, 0.0).astype(bf16)
        found = dot(window_hi[...], hot) + dot(window_lo[...], hot)
        y_mod = place // TILE_SIDE
        z_cell = place % TILE_SIDE
        z_iota = iota((TILE_SIDE, step), 0)
        at_z = (z_iota == z_cell, z_iota == z_cell + 1)
        corner = {}
        for a in range(2):
            parts = [found[a * 160 + TILE_SIDE * j : a * 160 + TILE_SIDE * (j + 1)] for j in range(5)]
            for b in range(2):
                rows_y = jnp.where(y_mod == 0, parts[b], 0.0)
                for j in range(1, 4):
                    rows_y = jnp.where(y_mod == j, parts[j + b], rows_y)
                for c in range(2):
                    corner[a, b, c] = jnp.sum(
                        jnp.where(at_z[c], rows_y, 0.0), axis=0, keepdims=True
                    )
        fr = [x[2:3], x[3:4], x[4:5]]
        w = [(1.0 - t, t) for t in fr]
        sign = (-1.0, 1.0)
        values = [jnp.zeros((1, step), f32) for _ in range(4)]
        for (a, b, c), k in corner.items():
            values[0] = values[0] + w[0][a] * w[1][b] * w[2][c] * k
            values[1] = values[1] + sign[a] * w[1][b] * w[2][c] * k
            values[2] = values[2] + w[0][a] * sign[b] * w[2][c] * k
            values[3] = values[3] + w[0][a] * w[1][b] * sign[c] * k
        du = [x[5:6], x[6:7], x[7:8]]
        lap = x[8:9]
        residual = (
            -(values[0] * lap + (values[1] * du[0] + values[2] * du[1] + values[3] * du[2]))
            - x[9:10]
        )
        scaled = 2.0 * x[10:11] * residual
        zeros = jnp.zeros((4, step), f32)
        answer = jnp.concatenate(values + [zeros], axis=0)
        sub = iota((8, LANES), 0)
        lane_of = iota((8, LANES), 1) // lanes_each
        for j in range(step // LANES):
            block = start // LANES + j
            part = answer[:, j * LANES : (j + 1) * LANES]
            turned = [pltpu.roll(part, lanes_each * k, 1) if k else part for k in range(group)]
            for g in range(group):
                picked = jnp.zeros((8, LANES), f32)
                for c in range(4):
                    picked = jnp.where((sub == c) & (lane_of == c), turned[(c - g) % group], picked)
                response_ref[group * block + g] = jnp.sum(picked, axis=0, keepdims=True)
        kept_ref[:, start : start + step] = jnp.concatenate(
            [x[0:5], -scaled * lap, -scaled * du[0], -scaled * du[1], -scaled * du[2]]
            + [jnp.zeros((7, step), f32)],
            axis=0,
        )


def spread_kernel(
    tiles,
    kept_ref, smooth_ref,
    grad_ref,
    hot_ref, c_hi, c_lo, sum_ref, part_ref,
):
    cells = smooth_ref.shape[0]
    slots = kept_ref.shape[1]
    plane = (TILE_SIDE // 4) * tiles
    step = 2 * LANES
    for start in range(0, slots, step):
        lanes = slice(start, start + step)
        x = kept_ref[:, lanes]
        rows = x[0:1].astype(jnp.int32)
        place = x[1:2].astype(jnp.int32)
        hot_ref[:, lanes] = jnp.where(iota((cells, step), 0) == rows, 1.0, 0.0).astype(bf16)
        y_mod = place // TILE_SIDE
        z_cell = place % TILE_SIDE
        z_iota = iota((TILE_SIDE, step), 0)
        at_z = (z_iota == z_cell, z_iota == z_cell + 1)
        w = [(1.0 - x[k : k + 1], x[k : k + 1]) for k in (2, 3, 4)]
        g = [x[k : k + 1] for k in (5, 6, 7, 8)]
        sign = (-1.0, 1.0)
        for a in range(2):
            along = []
            for b in range(2):
                pair = []
                for c in range(2):
                    pair.append(
                        g[0] * w[0][a] * w[1][b] * w[2][c]
                        + g[1] * sign[a] * w[1][b] * w[2][c]
                        + g[2] * w[0][a] * sign[b] * w[2][c]
                        + g[3] * w[0][a] * w[1][b] * sign[c]
                    )
                along.append(jnp.where(at_z[0], pair[0], 0.0) + jnp.where(at_z[1], pair[1], 0.0))
            for j in range(5):
                value = jnp.where(y_mod == j, along[0], 0.0) + jnp.where(
                    y_mod == j - 1, along[1], 0.0
                )
                hi, lo = split2(value)
                at = a * 128 + TILE_SIDE * j if j < 4 else 256 + a * TILE_SIDE
                c_hi[at : at + TILE_SIDE, lanes] = hi
                c_lo[at : at + TILE_SIDE, lanes] = lo
    sum_ref[...] = jnp.zeros(sum_ref.shape, f32)
    block = 2 * LANES
    for start in range(0, cells, block):
        hot = hot_ref[start : start + block, :]
        part = dot(hot, c_hi[...], NT) + dot(hot, c_lo[...], NT)
        part_ref[start : start + block, :] = part
    sum_ref[0:cells, :] = smooth_ref[...] + part_ref[:, 0:128]
    sum_ref[plane : plane + cells, :] += part_ref[:, 128:256]
    low = slice(0, TILE_SIDE)
    sum_ref[tiles : tiles + cells, low] += part_ref[:, 256 : 256 + TILE_SIDE]
    sum_ref[plane + tiles : plane + tiles + cells, low] += part_ref[
        :, 256 + TILE_SIDE : 256 + 2 * TILE_SIDE
    ]
    grad_ref[...] = sum_ref[0:cells, :]


def prepare_kernel(
    devices, tiles,
    index_ref, field_ref, before_ref, after_ref,
    grad_ref, energy_ref, window_hi, window_lo,
    padded_ref,
):
    cells = field_ref.shape[0]
    plane = (TILE_SIDE // 4) * tiles
    padded_ref[0:cells, :] = field_ref[...]
    padded_ref[cells:, :] = jnp.zeros((padded_ref.shape[0] - cells, LANES), f32)
    for a in range(2):
        base = a * plane
        main = jnp.transpose(padded_ref[base : base + cells, :])
        hi, lo = split2(main)
        window_hi[a * 160 : a * 160 + 128, :] = hi
        window_lo[a * 160 : a * 160 + 128, :] = lo
        extra = jnp.transpose(padded_ref[base + tiles : base + tiles + cells, :])[0:TILE_SIDE]
        hi, lo = split2(extra)
        window_hi[a * 160 + 128 : a * 160 + 160, :] = hi
        window_lo[a * 160 + 128 : a * 160 + 160, :] = lo

    me = index_ref[0, 0]
    row = iota((plane, LANES), 0)
    lane = iota((plane, LANES), 1)
    z_inner = (lane % TILE_SIDE) < TILE_SIDE - 1
    first_row = row < tiles
    last_row = row >= plane - tiles
    low_lane = lane < TILE_SIDE
    high_lane = lane >= LANES - TILE_SIDE
    has_after = jnp.where(me < devices - 1, 1.0, 0.0)
    has_before = jnp.where(me > 0, 1.0, 0.0)
    after_mask = jnp.where(last_row & high_lane, has_after, 1.0)
    before_mask = jnp.where(first_row & low_lane, has_before, 1.0)
    next_tile = (row % tiles) < tiles - 1
    prev_tile = (row % tiles) > 0

    def load(x):
        return field_ref[pl.ds(pl.multiple_of(x * plane, plane), plane), :]

    def plane_step(x, energy):
        here = load(x)
        diff_z = jnp.where(z_inner, pltpu.roll(here, LANES - 1, 1) - here, 0.0)
        grad = pltpu.roll(diff_z, 1, 1) - diff_z
        energy = energy + diff_z * diff_z
        above = jnp.concatenate([here[tiles:], after_ref[x]], axis=0)
        up = pltpu.roll(jnp.where(low_lane, above, here), LANES - TILE_SIDE, 1)
        below = jnp.concatenate([before_ref[x], here[: plane - tiles]], axis=0)
        down = pltpu.roll(jnp.where(high_lane, below, here), TILE_SIDE, 1)
        diff_up = (up - here) * after_mask
        diff_down = (here - down) * before_mask
        grad = grad + diff_down - diff_up
        energy = energy + diff_down * diff_down
        first = x == 0
        last = x == TILE_SIDE - 1
        nxt = load(jnp.where(last, 0, x + 1))
        nxt = jnp.where(last, pltpu.roll(nxt, plane - 1, 0), nxt)
        prv = load(jnp.where(first, TILE_SIDE - 1, x - 1))
        prv = jnp.where(first, pltpu.roll(prv, 1, 0), prv)
        diff_next = jnp.where(jnp.logical_not(last) | next_tile, nxt - here, 0.0)
        diff_prev = jnp.where(jnp.logical_not(first) | prev_tile, here - prv, 0.0)
        grad = grad + diff_prev - diff_next
        energy = energy + diff_prev * diff_prev
        at = pl.ds(pl.multiple_of(x * plane, plane), plane)
        grad_ref[at, :] = 2.0 * smooth_weight * grad
        return energy

    energy = lax.fori_loop(0, TILE_SIDE, plane_step, jnp.zeros((plane, LANES), f32))
    energy_ref[...] = jnp.sum(energy, axis=0, keepdims=True)


def backward_kernel(
    devices, layers, lanes_each,
    scalars_ref, owner_row_ref, source_ref, observed_ref, response_ref, energy_ref,
    outputs_ref, readout_ref, weights_hbm, pre_hbm, parts_hbm,
    keep_a_ref, keep_b_ref, send_a_ref, send_b_ref,
    pre_ref, parts_ref, weights_ref, bar_ref, zh_ref, zl_ref, col_ref, cols_ref, sems,
):
    def fetch_pre(k):
        return pltpu.make_async_copy(pre_hbm.at[k], pre_ref.at[k], sems.at[0, k])

    def fetch_parts(k):
        return pltpu.make_async_copy(parts_hbm.at[k], parts_ref.at[k], sems.at[1, k])

    weight_copy = pltpu.make_async_copy(weights_hbm, weights_ref, sems.at[0, layers])
    fetch_pre(layers - 1).start()
    weight_copy.start()
    fetch_parts(layers - 1).start()
    points = owner_row_ref.shape[1]
    width = weights_hbm.shape[1]
    owner_row = owner_row_ref[...]
    ranks = slot_ranks_row(column_of(owner_row), owner_row)
    picked = jnp.where(ranks == iota((lanes_each, points), 0), 1.0, 0.0)
    from_owner = jnp.where(owner_row == iota((devices, points), 0), 1.0, 0.0).astype(bf16)
    a, b, c = split3(jnp.transpose(response_ref[...])[0 : 4 * lanes_each])
    wide = dot(a, from_owner) + dot(b, from_owner) + dot(c, from_owner)
    values = [
        jnp.sum(picked * wide[k * lanes_each : (k + 1) * lanes_each], axis=0, keepdims=True)
        for k in range(4)
    ]
    outputs = outputs_ref[...]
    out = [outputs[k : k + 1] for k in range(5)]
    live = jnp.where(iota((1, points), 1) < scalars_ref[0, 0], 1.0, 0.0)
    misfit = out[0] - observed_ref[...]
    residual = (
        -(values[0] * out[4] + (values[1] * out[1] + values[2] * out[2] + values[3] * out[3]))
        - source_ref[...]
    )
    scaled = 2.0 * live * residual
    out_grad = [2.0 * data_weight * live * misfit] + [-scaled * values[k] for k in (1, 2, 3, 0)]
    residual_sum = jnp.sum(live * residual * residual, axis=1, keepdims=True)
    misfit_sum = jnp.sum(live * misfit * misfit, axis=1, keepdims=True)
    col_ref[...] = column_of(readout_ref[...])
    cols_ref[...] = jnp.zeros(cols_ref.shape, f32)
    lane8 = iota((ROWS, cols_ref.shape[1]), 1)
    chunks = width // ROWS

    def rows_of(c):
        return pl.ds(pl.multiple_of(c * ROWS, ROWS), ROWS)

    def pre_of(depth, rows):
        return [pre_ref[depth, rows, pl.ds(k * points, points)] for k in range(5)]

    def readout_chunk(c, carry):
        rows = rows_of(c)
        v, z1, z2, z3, z4 = pre_of(layers - 1, rows)
        s, _, curve = activations(v, z1, z2, z3, z4)
        total = out_grad[0] * v + out_grad[1] * (s * z1) + out_grad[2] * (s * z2)
        total = total + out_grad[3] * (s * z3) + out_grad[4] * curve
        grad = jnp.sum(total, axis=1, keepdims=True)
        cols_ref[rows, :] += jnp.where(lane8 == layers, grad, 0.0)
        r = col_ref[rows, :]
        for k in range(5):
            bar_ref[rows, pl.ds(k * points, points)] = r * out_grad[k]
        return carry

    fetch_pre(layers - 1).wait()
    lax.fori_loop(0, chunks, readout_chunk, 0)
    weight_copy.wait()
    mine = scalars_ref[0, 1]
    half = layers // 2

    def layer(step, carry):
        depth = layers - 1 - step
        before = jnp.maximum(depth - 1, 0)

        @pl.when(depth > 0)
        def _():
            fetch_pre(before).start()
            fetch_parts(before).start()

        def bars(c, inner):
            rows = rows_of(c)
            v, z1, z2, z3, z4 = pre_of(depth, rows)
            b = [bar_ref[rows, pl.ds(k * points, points)] for k in range(5)]
            s = 1.0 - v * v
            q = z1 * z1 + z2 * z2 + z3 * z3
            slope = b[1] * z1 + b[2] * z2 + b[3] * z3
            v4c = 4.0 * v * b[4]
            z_bar = [
                s
                * (
                    b[0]
                    - 2.0 * v * slope
                    + b[4] * (q * (4.0 * v * v - 2.0 * s) - 2.0 * v * z4)
                ),
                s * (b[1] - v4c * z1),
                s * (b[2] - v4c * z2),
                s * (b[3] - v4c * z3),
                s * b[4],
            ]
            grad = jnp.sum(z_bar[0], axis=1, keepdims=True)
            cols_ref[rows, :] += jnp.where(lane8 == depth, grad, 0.0)
            for k in range(5):
                lanes = pl.ds(k * points, points)
                hi, lo = split2(z_bar[k])
                zh_ref[rows, lanes] = hi
                zl_ref[rows, lanes] = lo
            return inner

        lax.fori_loop(0, chunks, bars, 0)
        fetch_parts(depth).wait()
        h_hi, h_lo = parts_ref[depth, 0:width], parts_ref[depth, width:]
        z_hi, z_lo = zh_ref[...], zl_ref[...]
        grad = dot(z_hi, h_hi, NT) + dot(z_hi, h_lo, NT) + dot(z_lo, h_hi, NT)
        upper = (depth >= half).astype(jnp.int32)
        part = width // 2
        at = pl.ds(pl.multiple_of((depth - upper * half) * part, part), part)

        @pl.when(mine == upper)
        def _():
            keep_a_ref[at, :] = grad[:part]
            keep_b_ref[at, :] = grad[part:]

        @pl.when(mine != upper)
        def _():
            send_a_ref[at, :] = grad[:part]
            send_b_ref[at, :] = grad[part:]

        @pl.when(depth > 0)
        def _():
            w_hi, w_lo = split2(jnp.transpose(weights_ref[depth]))
            for k in range(5):
                lanes = pl.ds(k * points, points)
                z_hi = zh_ref[:, lanes]
                bar_ref[:, lanes] = dot(w_hi, z_hi) + dot(w_hi, zl_ref[:, lanes]) + dot(w_lo, z_hi)
            fetch_pre(before).wait()

        return carry

    lax.fori_loop(0, layers, layer, 0)
    small = jnp.transpose(cols_ref[...])
    lane = iota((1, width), 1)
    count = jnp.full((1, 1), scalars_ref[0, 0], jnp.int32).astype(f32)
    last = jnp.where(lane == 0, residual_sum, 0.0) + jnp.where(lane == 1, misfit_sum, 0.0)
    energy = jnp.sum(energy_ref[...], axis=1, keepdims=True)
    last = last + jnp.where(lane == 2, count, 0.0) + jnp.where(lane == 3, energy, 0.0)
    small = jnp.where(iota(small.shape, 0) == small.shape[0] - 1, last, small)
    keep_b_ref[half * width // 2 :, :] = small
    send_b_ref[half * width // 2 :, :] = small


def vmem():
    return pl.BlockSpec(memory_space=pltpu.VMEM)


def smem():
    return pl.BlockSpec(memory_space=pltpu.SMEM)


def hbm():
    return pl.BlockSpec(memory_space=pltpu.HBM)


def call(kernel, name, specs, out_shapes, scratch, flops, limit, outs=None):
    return pl.pallas_call(
        kernel,
        name=name,
        out_shape=out_shapes,
        in_specs=specs,
        out_specs=outs or jax.tree.map(lambda _: vmem(), out_shapes),
        scratch_shapes=scratch,
        compiler_params=pltpu.CompilerParams(vmem_limit_bytes=min(limit << 20, 67043328)),
        cost_estimate=pl.CostEstimate(flops=flops, bytes_accessed=1 << 20, transcendentals=0),
    )


def shape(*dims, dtype=f32):
    return jax.ShapeDtypeStruct(dims, dtype)


def on_device(
    conductivity, owner_rank, tile_slot, offsets, fractions, source, observed, live_count,
    fourier, weights, biases, readout,
):
    devices = lax.axis_size(AXES)
    index = lax.axis_index(AXES)
    points = tile_slot.shape[0]
    tiles = conductivity.shape[0]
    layers, width = biases.shape
    capacity = (2 * points + devices - 1) // devices + 1
    lanes_each = 1 << (capacity - 1).bit_length()
    lanes_each = max(lanes_each, 2 * LANES // devices)
    rows_each = 1 << (-(-11 * lanes_each // LANES) - 1).bit_length()
    slots = devices * lanes_each
    cells = conductivity.size // LANES
    plane = (TILE_SIDE // 4) * tiles
    wide = 5 * points

    owner_row = owner_rank.reshape(1, points)
    source_row = source.reshape(1, points)
    readout_row = readout.reshape(1, width)
    field = conductivity.reshape(tiles, cells // tiles, LANES).transpose(1, 0, 2)
    field = field.reshape(cells, LANES)

    request, outputs, pre, parts = call(
        functools.partial(forward_kernel, devices, layers, tiles, lanes_each),
        "forward",
        [smem()] + [hbm()] * 9,
        (
            shape(devices, rows_each, LANES), shape(8, points),
            shape(layers, width, wide), shape(layers, 2 * width, wide, dtype=bf16),
        ),
        [
            pltpu.VMEM((layers, width, wide), f32),
            pltpu.VMEM((layers + 1, 2 * width, wide), bf16),
            pltpu.VMEM((layers, width, width), f32),
            pltpu.VMEM((width, wide), f32),
            pltpu.VMEM((width, 8), f32),
            pltpu.VMEM((width, 1), f32),
            pltpu.VMEM((1, points), jnp.int32),
            pltpu.VMEM((1, points), jnp.int32),
            pltpu.VMEM((3, points), jnp.int32),
            pltpu.VMEM((3, points), f32),
            pltpu.VMEM((1, points), f32),
            pltpu.VMEM((8, fourier.shape[0]), f32),
            pltpu.VMEM((8, width), f32),
            pltpu.VMEM((3, fourier.shape[0]), f32),
            pltpu.VMEM((layers, width), f32),
            pltpu.VMEM((1, width), f32),
            pltpu.SemaphoreType.DMA((9,)),
            pltpu.SemaphoreType.DMA((2, layers)),
        ],
        6 * 2 * layers * width * width * wide,
        FORWARD_LIMIT,
        outs=(vmem(), vmem(), hbm(), hbm()),
    )(
        live_count.reshape(1, 1), owner_row, tile_slot.reshape(1, points), offsets, fractions,
        source_row, fourier.T, weights, biases, readout_row,
    )
    received = lax.all_to_all(request, AXES, split_axis=0, concat_axis=0, tiled=True)

    planes, _ = lax.optimization_barrier((field.reshape(TILE_SIDE, plane, LANES), outputs))
    up = [(i, i + 1) for i in range(devices - 1)]
    down = [(j, i) for i, j in up]
    before = lax.ppermute(planes[:, plane - tiles :, :], AXES, up)
    after = lax.ppermute(planes[:, :tiles, :], AXES, down)
    smooth, energy, window_hi, window_lo = call(
        functools.partial(prepare_kernel, devices, tiles),
        "prepare",
        [smem()] + [vmem()] * 3,
        (
            shape(cells, LANES), shape(1, LANES),
            shape(320, cells, dtype=bf16), shape(320, cells, dtype=bf16),
        ),
        [pltpu.VMEM((cells + 2 * plane, LANES), f32)],
        FILL,
        PREPARE_LIMIT,
    )(index.reshape(1, 1), field, before, after)

    response, kept = call(
        functools.partial(owner_kernel, devices, tiles, lanes_each),
        "lookup",
        [vmem()] * 3,
        (shape(devices, 1, LANES), shape(16, slots)),
        [pltpu.VMEM((16, slots), f32)],
        2 * 640 * cells * slots,
        LOOKUP_LIMIT,
    )(received, window_hi, window_lo)
    answered = lax.all_to_all(response, AXES, split_axis=0, concat_axis=0, tiled=True)
    grad = call(
        functools.partial(spread_kernel, tiles),
        "spread",
        [vmem()] * 2,
        shape(cells, LANES),
        [
            pltpu.VMEM((cells, slots), bf16),
            pltpu.VMEM((320, slots), bf16),
            pltpu.VMEM((320, slots), bf16),
            pltpu.VMEM((cells + 2 * plane, LANES), f32),
            pltpu.VMEM((cells, 320), f32),
        ],
        FILL,
        SPREAD_LIMIT,
    )(kept, smooth)
    answered, grad = lax.optimization_barrier((answered, grad))

    part_rows = layers * width // 4
    scalars = jnp.stack([live_count[0], index % 2]).reshape(1, 2)
    keep_a, keep_b, send_a, send_b = call(
        functools.partial(backward_kernel, devices, layers, lanes_each),
        "backward",
        [smem()] + [vmem()] * 7 + [hbm()] * 3,
        tuple(shape(rows, width) for rows in (part_rows, part_rows + 8) * 2),
        [
            pltpu.VMEM((layers, width, wide), f32),
            pltpu.VMEM((layers, 2 * width, wide), bf16),
            pltpu.VMEM((layers, width, width), f32),
            pltpu.VMEM((width, wide), f32),
            pltpu.VMEM((width, wide), bf16),
            pltpu.VMEM((width, wide), bf16),
            pltpu.VMEM((width, 1), f32),
            pltpu.VMEM((width, 8), f32),
            pltpu.SemaphoreType.DMA((2, layers + 1)),
        ],
        12 * 2 * layers * width * width * wide,
        BACKWARD_LIMIT,
    )(
        scalars, owner_row, source_row, observed.reshape(1, points),
        answered.reshape(devices, LANES), energy, outputs, readout_row, weights, pre, parts,
    )

    even = [1 << k for k in range(devices.bit_length() - 1)]
    odd = list(even)
    for k in range(1, len(odd) - 1, 2):
        odd[k], odd[k + 1] = odd[k + 1], odd[k]

    def exchange(value, step):
        bits = (even[step], odd[step])
        return lax.ppermute(value, AXES, [(i, i ^ bits[i % 2]) for i in range(devices)])

    def upper_of(step):
        bit = jnp.where(index % 2 == 1, odd[step], even[step])
        return (index & bit) != 0

    main = [keep_a + exchange(send_a, 0), keep_b + exchange(send_b, 0)]
    main[1], extra = main[1][:part_rows], main[1][part_rows:]
    for step in range(1, len(even)):
        half = main[0].shape[0] // 2
        upper = upper_of(step)
        outgoing = [jnp.where(upper, m[:half], m[half:]) for m in main]
        outgoing[1] = jnp.concatenate([outgoing[1], extra], axis=0)
        arrived = [exchange(value, step) for value in outgoing]
        main = [jnp.where(upper, m[half:], m[:half]) + a[:half] for m, a in zip(main, arrived)]
        extra = extra + arrived[1][half:]
    scale = 1.0 / extra[7, 2]
    main = [m * scale for m in main]
    sums = extra[7]
    losses = jnp.stack(
        [sums[0] * scale, sums[1] * scale, sums[3] / (devices * conductivity.size)]
    )
    bias_grad, readout_grad = extra[:layers] * scale, extra[layers] * scale
    for step in reversed(range(len(even))):
        upper = upper_of(step)
        arrived = [exchange(m, step) for m in main]
        main = [
            jnp.concatenate([jnp.where(upper, a, m), jnp.where(upper, m, a)], axis=0)
            for m, a in zip(main, arrived)
        ]
        if step == len(even) - 1:
            main[1], losses, bias_grad, readout_grad = lax.optimization_barrier(
                (main[1], losses, bias_grad, readout_grad)
            )
    weight_grad = jnp.concatenate([m.reshape(layers, width // 2, width) for m in main], axis=1)
    conductivity_grad = grad.reshape(cells // tiles, tiles, LANES).transpose(1, 0, 2)
    return (
        conductivity_grad.reshape(conductivity.shape),
        weight_grad,
        bias_grad,
        readout_grad,
        losses,
    )


def solution(mesh):
    in_specs = (
        P(AXES, None), P(AXES, None), P(AXES), P(None, AXES), P(None, AXES), P(AXES), P(AXES),
        P(AXES), P(), P(), P(), P(),
    )
    out_specs = (P(AXES, None), P(), P(), P(), P())
    return jax.shard_map(
        on_device, mesh=mesh, in_specs=in_specs, out_specs=out_specs, check_vma=False
    )
```

```python
import functools

import jax
import jax.numpy as jnp
from jax import lax
from jax.experimental import pallas as pl
from jax.experimental.pallas import tpu as pltpu
from jax.sharding import PartitionSpec as P

TILE_SIDE = 32
LANES = 128
data_weight = 1.0
smooth_weight = 0.05
AXES = ("gx", "gy")
f32 = jnp.float32
bf16 = jnp.bfloat16
NN = (((1,), (0,)), ((), ()))
NT = (((1,), (1,)), ((), ()))


def dot(a, b, dims=NN):
    return lax.dot_general(a, b, dims, preferred_element_type=f32)


def split2(x):
    hi = x.astype(bf16)
    return hi, (x - hi.astype(f32)).astype(bf16)


def split3(x):
    hi = x.astype(bf16)
    rest = x - hi.astype(f32)
    mid = rest.astype(bf16)
    return hi, mid, (rest - mid.astype(f32)).astype(bf16)


def iota(shape, dim):
    return lax.broadcasted_iota(jnp.int32, shape, dim)


def sin_cos(phase):
    turns = jnp.floor(phase * 0.6366197723675814 + 0.5)
    y = phase - turns * 1.5703125
    y = y - turns * 4.837512969970703125e-4
    y = y - turns * 7.549789954891882e-8
    quarter = turns.astype(jnp.int32)
    y2 = y * y
    s = y + y * y2 * (-1.6666654611e-1 + y2 * (8.3321608736e-3 - y2 * 1.9515295891e-4))
    c = (
        1.0
        - 0.5 * y2
        + y2
        * y2
        * (4.166664568298827e-2 + y2 * (-1.388731625493765e-3 + y2 * 2.443315711809948e-5))
    )
    odd = (quarter & 1) == 1
    sin_part = jnp.where(odd, c, s)
    cos_part = jnp.where(odd, s, c)
    sin_part = jnp.where((quarter & 2) == 2, -sin_part, sin_part)
    cos_part = jnp.where(((quarter + 1) & 2) == 2, -cos_part, cos_part)
    return sin_part, cos_part


def activations(v, z1, z2, z3, z4):
    s = 1.0 - v * v
    q = z1 * z1 + z2 * z2 + z3 * z3
    return s, q, s * z4 - 2.0 * v * s * q


def column_of(row):
    wide = jnp.broadcast_to(row.astype(f32), (8, row.shape[1]))
    return jnp.transpose(wide)[:, 0:1].astype(row.dtype)


def slot_ranks_row(owner_col, owner_row):
    n = owner_row.shape[1]
    same = (owner_col == owner_row) & (iota((n, n), 0) < iota((n, n), 1))
    return jnp.sum(jnp.where(same, 1.0, 0.0), axis=0, keepdims=True).astype(jnp.int32)


def slot_ranks_col(owner_col, owner_row):
    n = owner_row.shape[1]
    same = (owner_col == owner_row) & (iota((n, n), 1) < iota((n, n), 0))
    return jnp.sum(jnp.where(same, 1.0, 0.0), axis=1, keepdims=True).astype(jnp.int32)


FORWARD_ROWS, ROWS = 256, 64
FILL = 4 * 10**9
FORWARD_LIMIT, PREPARE_LIMIT, LOOKUP_LIMIT, SPREAD_LIMIT, BACKWARD_LIMIT = 64, 8, 12, 14, 58


def forward_kernel(
    devices, layers, tiles, lanes_each,
    live_ref, owner_hbm, slot_hbm, offsets_hbm, fractions_hbm, source_hbm,
    fourier_hbm, weights_hbm, biases_hbm, readout_hbm,
    request_ref, outputs_ref, pre_hbm, parts_hbm,
    pre_ref, parts_ref, weights_ref, z_ref, col_ref, bias_ref,
    owner_ref, slot_ref, offsets_ref, fractions_ref, source_ref, fourier_ref, small_ref,
    freq_ref, biases_ref, readout_ref, sems, out_sems,
):
    small_ref[...] = jnp.zeros(small_ref.shape, f32)
    fourier_ref[...] = jnp.zeros(fourier_ref.shape, f32)
    copies = [
        pltpu.make_async_copy(source, target, sems.at[k])
        for k, (source, target) in enumerate(
            (
                (owner_hbm, owner_ref), (slot_hbm, slot_ref), (offsets_hbm, offsets_ref),
                (fractions_hbm, fractions_ref), (fourier_hbm, freq_ref),
                (source_hbm, source_ref), (biases_hbm, biases_ref),
                (readout_hbm, readout_ref), (weights_hbm, weights_ref),
            )
        )
    ]
    for copy in copies:
        copy.start()
    for copy in copies[:-1]:
        copy.wait()
    fourier_ref[0:3, :] = freq_ref[...]
    small_ref[0:layers, :] = biases_ref[...]
    small_ref[layers : layers + 1, :] = readout_ref[...]
    points = slot_ref.shape[1]
    width = weights_ref.shape[1]
    streams = 5
    off = offsets_ref[...]
    fractions = fractions_ref[...]
    owner_row = owner_ref[...]
    slot = slot_ref[...]
    cells = jnp.concatenate(
        [TILE_SIDE * slot + off[0:1], TILE_SIDE * owner_row + off[1:2], off[2:3]], axis=0
    )
    position = cells.astype(f32) + fractions
    f = jnp.transpose(fourier_ref[...])
    phases = f[:, 0:1] * position[0:1] + f[:, 1:2] * position[1:2] + f[:, 2:3] * position[2:3]
    sin_part, cos_part = sin_cos(phases)
    squared = f[:, 0:1] * f[:, 0:1] + f[:, 1:2] * f[:, 1:2] + f[:, 2:3] * f[:, 2:3]
    freqs = f.shape[0]

    def put(stream, top, bottom):
        for start, value in ((0, top), (freqs, bottom)):
            lanes = pl.ds(stream * points, points)
            hi, lo = split2(value)
            parts_ref[0, pl.ds(start, freqs), lanes] = hi
            parts_ref[0, pl.ds(width + start, freqs), lanes] = lo

    put(0, sin_part, cos_part)
    for k in range(3):
        put(k + 1, cos_part * f[:, k : k + 1], -sin_part * f[:, k : k + 1])
    put(4, -sin_part * squared, -cos_part * squared)

    small_cols = jnp.transpose(small_ref[...])
    col_ref[...] = small_cols
    copies[-1].wait()

    def leave_parts(depth):
        return pltpu.make_async_copy(
            parts_ref.at[depth], parts_hbm.at[depth], out_sems.at[0, depth]
        )

    def leave_pre(depth):
        return pltpu.make_async_copy(pre_ref.at[depth], pre_hbm.at[depth], out_sems.at[1, depth])

    def layer(depth, carry):
        leave_parts(depth).start()
        w_hi, w_lo = split2(weights_ref[depth])
        for k in range(streams):
            lanes = pl.ds(k * points, points)
            h_hi = parts_ref[depth, 0:width, lanes]
            h_lo = parts_ref[depth, width:, lanes]
            z_ref[:, lanes] = dot(w_hi, h_hi) + dot(w_hi, h_lo) + dot(w_lo, h_hi)
        bias = jnp.sum(
            jnp.where(iota(small_cols.shape, 1) == depth, small_cols, 0.0), axis=1, keepdims=True
        )
        bias_ref[...] = bias

        def chunk(c, inner):
            rows = pl.ds(pl.multiple_of(c * FORWARD_ROWS, FORWARD_ROWS), FORWARD_ROWS)
            low_rows = pl.ds(pl.multiple_of(width + c * FORWARD_ROWS, FORWARD_ROWS), FORWARD_ROWS)

            def z_of(k):
                return z_ref[rows, pl.ds(k * points, points)]

            v = jnp.tanh(z_of(0) + bias_ref[rows, :])
            z1, z2, z3, z4 = z_of(1), z_of(2), z_of(3), z_of(4)
            s, _, curve = activations(v, z1, z2, z3, z4)
            for k, (kept, h) in enumerate(
                ((v, v), (z1, s * z1), (z2, s * z2), (z3, s * z3), (z4, curve))
            ):
                lanes = pl.ds(k * points, points)
                pre_ref[depth, rows, lanes] = kept
                hi, lo = split2(h)
                parts_ref[depth + 1, rows, lanes] = hi
                parts_ref[depth + 1, low_rows, lanes] = lo
            return inner

        lax.fori_loop(0, width // FORWARD_ROWS, chunk, 0)
        leave_pre(depth).start()
        return carry

    lax.fori_loop(0, layers, layer, 0)

    def readout_chunk(c, totals):
        rows = pl.ds(pl.multiple_of(c * FORWARD_ROWS, FORWARD_ROWS), FORWARD_ROWS)
        v, z1, z2, z3, z4 = [
            pre_ref[layers - 1, rows, pl.ds(k * points, points)] for k in range(streams)
        ]
        s, _, curve = activations(v, z1, z2, z3, z4)
        r = col_ref[rows, layers : layers + 1]
        hs = (v, s * z1, s * z2, s * z3, curve)
        return tuple(t + jnp.sum(r * h, axis=0, keepdims=True) for t, h in zip(totals, hs))

    zero = tuple(jnp.zeros((1, points), f32) for _ in range(streams))
    out = lax.fori_loop(0, width // FORWARD_ROWS, readout_chunk, zero)
    outputs = jnp.concatenate(list(out) + [jnp.zeros((3, points), f32)], axis=0)
    outputs_ref[...] = outputs

    live = jnp.where(iota((1, points), 1) < live_ref[0, 0], 1.0, 0.0)
    row_index = ((off[0:1] * (TILE_SIDE // 4) + off[1:2] // 4) * tiles + slot).astype(f32)
    lane_index = ((off[1:2] % 4) * TILE_SIDE + off[2:3]).astype(f32)
    comps = [
        row_index, lane_index, fractions[0:1], fractions[1:2], fractions[2:3],
        outputs[1:2], outputs[2:3], outputs[3:4], outputs[4:5], source_ref[...], live,
    ]
    to_owner = owner_row == iota((devices, points), 0)
    ranks = slot_ranks_col(column_of(owner_row), owner_row)
    place = jnp.where(ranks == iota((points, LANES), 1), 1.0, 0.0).astype(bf16)
    spread = jnp.concatenate([jnp.where(to_owner, c, 0.0) for c in comps], axis=0)
    a, b, c = split3(spread)
    packed = dot(a, place) + dot(b, place) + dot(c, place)
    rows_each, lane_groups = request_ref.shape[1], LANES // lanes_each
    for j in range(rows_each):
        total = jnp.zeros((devices, LANES), f32)
        for m in range(lane_groups):
            k = rows_each * m + j
            if k < len(comps):
                part = packed[k * devices : (k + 1) * devices]
                total = total + (pltpu.roll(part, lanes_each * m, 1) if m else part)
        request_ref[:, j, :] = total
    for depth in range(layers):
        leave_parts(depth).wait()
        leave_pre(depth).wait()


def owner_kernel(
    devices, tiles, lanes_each,
    received_ref, window_hi, window_lo,
    response_ref, kept_ref,
    x_ref,
):
    cells = window_hi.shape[1]
    group = LANES // lanes_each
    blocks = devices // group
    slots = blocks * LANES
    rows_each = received_ref.shape[1]
    lane_block = iota((rows_each * group, LANES), 1) // lanes_each
    for j in range(blocks):
        total = None
        for g in range(group):
            part = received_ref[group * j + g]
            moved = jnp.concatenate(
                [
                    pltpu.roll(part, lanes_each * ((g - m) % group), 1) if g != m else part
                    for m in range(group)
                ],
                axis=0,
            )
            total = moved if total is None else jnp.where(lane_block == g, moved, total)
        x_ref[:, j * LANES : (j + 1) * LANES] = total

    step = 2 * LANES
    for start in range(0, slots, step):
        x = x_ref[:, start : start + step]
        rows = x[0:1].astype(jnp.int32)
        place = x[1:2].astype(jnp.int32)
        hot = jnp.where(iota((cells, step), 0) == rows, 1.0, 0.0).astype(bf16)
        found = dot(window_hi[...], hot) + dot(window_lo[...], hot)
        y_mod = place // TILE_SIDE
        z_cell = place % TILE_SIDE
        z_iota = iota((TILE_SIDE, step), 0)
        at_z = (z_iota == z_cell, z_iota == z_cell + 1)
        corner = {}
        for a in range(2):
            parts = [found[a * 160 + TILE_SIDE * j : a * 160 + TILE_SIDE * (j + 1)] for j in range(5)]
            for b in range(2):
                rows_y = jnp.where(y_mod == 0, parts[b], 0.0)
                for j in range(1, 4):
                    rows_y = jnp.where(y_mod == j, parts[j + b], rows_y)
                for c in range(2):
                    corner[a, b, c] = jnp.sum(
                        jnp.where(at_z[c], rows_y, 0.0), axis=0, keepdims=True
                    )
        fr = [x[2:3], x[3:4], x[4:5]]
        w = [(1.0 - t, t) for t in fr]
        sign = (-1.0, 1.0)
        values = [jnp.zeros((1, step), f32) for _ in range(4)]
        for (a, b, c), k in corner.items():
            values[0] = values[0] + w[0][a] * w[1][b] * w[2][c] * k
            values[1] = values[1] + sign[a] * w[1][b] * w[2][c] * k
            values[2] = values[2] + w[0][a] * sign[b] * w[2][c] * k
            values[3] = values[3] + w[0][a] * w[1][b] * sign[c] * k
        du = [x[5:6], x[6:7], x[7:8]]
        lap = x[8:9]
        residual = (
            -(values[0] * lap + (values[1] * du[0] + values[2] * du[1] + values[3] * du[2]))
            - x[9:10]
        )
        scaled = 2.0 * x[10:11] * residual
        zeros = jnp.zeros((4, step), f32)
        answer = jnp.concatenate(values + [zeros], axis=0)
        sub = iota((8, LANES), 0)
        lane_of = iota((8, LANES), 1) // lanes_each
        for j in range(step // LANES):
            block = start // LANES + j
            part = answer[:, j * LANES : (j + 1) * LANES]
            turned = [pltpu.roll(part, lanes_each * k, 1) if k else part for k in range(group)]
            for g in range(group):
                picked = jnp.zeros((8, LANES), f32)
                for c in range(4):
                    picked = jnp.where((sub == c) & (lane_of == c), turned[(c - g) % group], picked)
                response_ref[group * block + g] = jnp.sum(picked, axis=0, keepdims=True)
        kept_ref[:, start : start + step] = jnp.concatenate(
            [x[0:5], -scaled * lap, -scaled * du[0], -scaled * du[1], -scaled * du[2]]
            + [jnp.zeros((7, step), f32)],
            axis=0,
        )


def field_kernel(
    devices, tiles,
    index_ref, kept_ref, field_ref, before_ref, after_ref,
    grad_ref, energy_ref,
    hot_ref, c_hi, c_lo, sum_ref, part_ref,
):
    cells = field_ref.shape[0]
    slots = kept_ref.shape[1]
    plane = (TILE_SIDE // 4) * tiles
    step = 2 * LANES
    for start in range(0, slots, step):
        lanes = slice(start, start + step)
        x = kept_ref[:, lanes]
        rows = x[0:1].astype(jnp.int32)
        place = x[1:2].astype(jnp.int32)
        hot_ref[:, lanes] = jnp.where(iota((cells, step), 0) == rows, 1.0, 0.0).astype(bf16)
        y_mod = place // TILE_SIDE
        z_cell = place % TILE_SIDE
        z_iota = iota((TILE_SIDE, step), 0)
        at_z = (z_iota == z_cell, z_iota == z_cell + 1)
        w = [(1.0 - x[k : k + 1], x[k : k + 1]) for k in (2, 3, 4)]
        g = [x[k : k + 1] for k in (5, 6, 7, 8)]
        sign = (-1.0, 1.0)
        for a in range(2):
            along = []
            for b in range(2):
                pair = []
                for c in range(2):
                    pair.append(
                        g[0] * w[0][a] * w[1][b] * w[2][c]
                        + g[1] * sign[a] * w[1][b] * w[2][c]
                        + g[2] * w[0][a] * sign[b] * w[2][c]
                        + g[3] * w[0][a] * w[1][b] * sign[c]
                    )
                along.append(jnp.where(at_z[0], pair[0], 0.0) + jnp.where(at_z[1], pair[1], 0.0))
            for j in range(5):
                value = jnp.where(y_mod == j, along[0], 0.0) + jnp.where(
                    y_mod == j - 1, along[1], 0.0
                )
                hi, lo = split2(value)
                at = a * 128 + TILE_SIDE * j if j < 4 else 256 + a * TILE_SIDE
                c_hi[at : at + TILE_SIDE, lanes] = hi
                c_lo[at : at + TILE_SIDE, lanes] = lo
    sum_ref[...] = jnp.zeros(sum_ref.shape, f32)
    block = 2 * LANES
    for start in range(0, cells, block):
        hot = hot_ref[start : start + block, :]
        part = dot(hot, c_hi[...], NT) + dot(hot, c_lo[...], NT)
        part_ref[start : start + block, :] = part
    sum_ref[0:cells, :] = part_ref[:, 0:128]
    sum_ref[plane : plane + cells, :] += part_ref[:, 128:256]
    low = slice(0, TILE_SIDE)
    sum_ref[tiles : tiles + cells, low] += part_ref[:, 256 : 256 + TILE_SIDE]
    sum_ref[plane + tiles : plane + tiles + cells, low] += part_ref[
        :, 256 + TILE_SIDE : 256 + 2 * TILE_SIDE
    ]

    me = index_ref[0, 0]
    row = iota((plane, LANES), 0)
    lane = iota((plane, LANES), 1)
    z_inner = (lane % TILE_SIDE) < TILE_SIDE - 1
    first_row = row < tiles
    last_row = row >= plane - tiles
    low_lane = lane < TILE_SIDE
    high_lane = lane >= LANES - TILE_SIDE
    has_after = jnp.where(me < devices - 1, 1.0, 0.0)
    has_before = jnp.where(me > 0, 1.0, 0.0)
    after_mask = jnp.where(last_row & high_lane, has_after, 1.0)
    before_mask = jnp.where(first_row & low_lane, has_before, 1.0)
    next_tile = (row % tiles) < tiles - 1
    prev_tile = (row % tiles) > 0

    def load(x):
        return field_ref[pl.ds(pl.multiple_of(x * plane, plane), plane), :]

    def plane_step(x, energy):
        here = load(x)
        diff_z = jnp.where(z_inner, pltpu.roll(here, LANES - 1, 1) - here, 0.0)
        grad = pltpu.roll(diff_z, 1, 1) - diff_z
        energy = energy + diff_z * diff_z
        above = jnp.concatenate([here[tiles:], after_ref[x]], axis=0)
        up = pltpu.roll(jnp.where(low_lane, above, here), LANES - TILE_SIDE, 1)
        below = jnp.concatenate([before_ref[x], here[: plane - tiles]], axis=0)
        down = pltpu.roll(jnp.where(high_lane, below, here), TILE_SIDE, 1)
        diff_up = (up - here) * after_mask
        diff_down = (here - down) * before_mask
        grad = grad + diff_down - diff_up
        energy = energy + diff_down * diff_down
        first = x == 0
        last = x == TILE_SIDE - 1
        nxt = load(jnp.where(last, 0, x + 1))
        nxt = jnp.where(last, pltpu.roll(nxt, plane - 1, 0), nxt)
        prv = load(jnp.where(first, TILE_SIDE - 1, x - 1))
        prv = jnp.where(first, pltpu.roll(prv, 1, 0), prv)
        diff_next = jnp.where(jnp.logical_not(last) | next_tile, nxt - here, 0.0)
        diff_prev = jnp.where(jnp.logical_not(first) | prev_tile, here - prv, 0.0)
        grad = grad + diff_prev - diff_next
        energy = energy + diff_prev * diff_prev
        at = pl.ds(pl.multiple_of(x * plane, plane), plane)
        grad_ref[at, :] = sum_ref[at, :] + 2.0 * smooth_weight * grad
        return energy

    energy = lax.fori_loop(
        0, TILE_SIDE, plane_step, jnp.zeros((plane, LANES), f32), unroll=4
    )
    energy_ref[...] = jnp.sum(energy, axis=0, keepdims=True)


def prepare_kernel(
    tiles,
    field_ref,
    window_hi, window_lo, first_ref, last_ref,
    padded_ref,
):
    cells = field_ref.shape[0]
    plane = (TILE_SIDE // 4) * tiles
    for x in range(TILE_SIDE):
        first_ref[x] = field_ref[x * plane : x * plane + tiles, :]
        last_ref[x] = field_ref[(x + 1) * plane - tiles : (x + 1) * plane, :]
    padded_ref[0:cells, :] = field_ref[...]
    padded_ref[cells:, :] = jnp.zeros((padded_ref.shape[0] - cells, LANES), f32)
    for a in range(2):
        base = a * plane
        main = jnp.transpose(padded_ref[base : base + cells, :])
        hi, lo = split2(main)
        window_hi[a * 160 : a * 160 + 128, :] = hi
        window_lo[a * 160 : a * 160 + 128, :] = lo
        extra = jnp.transpose(padded_ref[base + tiles : base + tiles + cells, :])[0:TILE_SIDE]
        hi, lo = split2(extra)
        window_hi[a * 160 + 128 : a * 160 + 160, :] = hi
        window_lo[a * 160 + 128 : a * 160 + 160, :] = lo


def backward_kernel(
    devices, layers, lanes_each,
    live_ref, index_ref, owner_row_ref, source_ref, observed_ref, response_ref, energy_ref,
    outputs_ref, readout_ref, weights_hbm, pre_hbm, parts_hbm,
    keep_a_ref, keep_b_ref, send_a_ref, send_b_ref,
    pre_ref, parts_ref, weights_ref, bar_ref, zh_ref, zl_ref, col_ref, cols_ref, sems,
):
    def fetch_pre(k):
        return pltpu.make_async_copy(pre_hbm.at[k], pre_ref.at[k], sems.at[0, k])

    def fetch_parts(k):
        return pltpu.make_async_copy(parts_hbm.at[k], parts_ref.at[k], sems.at[1, k])

    weight_copy = pltpu.make_async_copy(weights_hbm, weights_ref, sems.at[0, layers])
    fetch_pre(layers - 1).start()
    weight_copy.start()
    fetch_parts(layers - 1).start()
    points = owner_row_ref.shape[1]
    width = weights_hbm.shape[1]
    owner_row = owner_row_ref[...]
    ranks = slot_ranks_row(column_of(owner_row), owner_row)
    picked = jnp.where(ranks == iota((lanes_each, points), 0), 1.0, 0.0)
    from_owner = jnp.where(owner_row == iota((devices, points), 0), 1.0, 0.0).astype(bf16)
    a, b, c = split3(jnp.transpose(response_ref[...])[0 : 4 * lanes_each])
    wide = dot(a, from_owner) + dot(b, from_owner) + dot(c, from_owner)
    values = [
        jnp.sum(picked * wide[k * lanes_each : (k + 1) * lanes_each], axis=0, keepdims=True)
        for k in range(4)
    ]
    outputs = outputs_ref[...]
    out = [outputs[k : k + 1] for k in range(5)]
    live = jnp.where(iota((1, points), 1) < live_ref[0, 0], 1.0, 0.0)
    misfit = out[0] - observed_ref[...]
    residual = (
        -(values[0] * out[4] + (values[1] * out[1] + values[2] * out[2] + values[3] * out[3]))
        - source_ref[...]
    )
    scaled = 2.0 * live * residual
    out_grad = [2.0 * data_weight * live * misfit] + [-scaled * values[k] for k in (1, 2, 3, 0)]
    residual_sum = jnp.sum(live * residual * residual, axis=1, keepdims=True)
    misfit_sum = jnp.sum(live * misfit * misfit, axis=1, keepdims=True)
    col_ref[...] = column_of(readout_ref[...])
    cols_ref[...] = jnp.zeros(cols_ref.shape, f32)
    lane8 = iota((ROWS, cols_ref.shape[1]), 1)
    chunks = width // ROWS

    def rows_of(c):
        return pl.ds(pl.multiple_of(c * ROWS, ROWS), ROWS)

    def pre_of(depth, rows):
        return [pre_ref[depth, rows, pl.ds(k * points, points)] for k in range(5)]

    def readout_chunk(c, carry):
        rows = rows_of(c)
        v, z1, z2, z3, z4 = pre_of(layers - 1, rows)
        s, _, curve = activations(v, z1, z2, z3, z4)
        total = out_grad[0] * v + out_grad[1] * (s * z1) + out_grad[2] * (s * z2)
        total = total + out_grad[3] * (s * z3) + out_grad[4] * curve
        grad = jnp.sum(total, axis=1, keepdims=True)
        cols_ref[rows, :] += jnp.where(lane8 == layers, grad, 0.0)
        r = col_ref[rows, :]
        for k in range(5):
            bar_ref[rows, pl.ds(k * points, points)] = r * out_grad[k]
        return carry

    fetch_pre(layers - 1).wait()
    lax.fori_loop(0, chunks, readout_chunk, 0)
    weight_copy.wait()
    mine = index_ref[0, 0] % 2
    half = layers // 2

    def layer(step, carry):
        depth = layers - 1 - step
        before = jnp.maximum(depth - 1, 0)

        @pl.when(depth > 0)
        def _():
            fetch_pre(before).start()
            fetch_parts(before).start()

        def bars(c, inner):
            rows = rows_of(c)
            v, z1, z2, z3, z4 = pre_of(depth, rows)
            b = [bar_ref[rows, pl.ds(k * points, points)] for k in range(5)]
            s = 1.0 - v * v
            q = z1 * z1 + z2 * z2 + z3 * z3
            slope = b[1] * z1 + b[2] * z2 + b[3] * z3
            v4c = 4.0 * v * b[4]
            z_bar = [
                s
                * (
                    b[0]
                    - 2.0 * v * slope
                    + b[4] * (q * (4.0 * v * v - 2.0 * s) - 2.0 * v * z4)
                ),
                s * (b[1] - v4c * z1),
                s * (b[2] - v4c * z2),
                s * (b[3] - v4c * z3),
                s * b[4],
            ]
            grad = jnp.sum(z_bar[0], axis=1, keepdims=True)
            cols_ref[rows, :] += jnp.where(lane8 == depth, grad, 0.0)
            for k in range(5):
                lanes = pl.ds(k * points, points)
                hi, lo = split2(z_bar[k])
                zh_ref[rows, lanes] = hi
                zl_ref[rows, lanes] = lo
            return inner

        lax.fori_loop(0, chunks, bars, 0, unroll=2)
        fetch_parts(depth).wait()
        h_hi, h_lo = parts_ref[depth, 0:width], parts_ref[depth, width:]
        z_hi, z_lo = zh_ref[...], zl_ref[...]
        grad = dot(z_hi, h_hi, NT) + dot(z_hi, h_lo, NT) + dot(z_lo, h_hi, NT)
        upper = (depth >= half).astype(jnp.int32)
        part = width // 2
        at = pl.ds(pl.multiple_of((depth - upper * half) * part, part), part)

        @pl.when(mine == upper)
        def _():
            keep_a_ref[at, :] = grad[:part]
            keep_b_ref[at, :] = grad[part:]

        @pl.when(mine != upper)
        def _():
            send_a_ref[at, :] = grad[:part]
            send_b_ref[at, :] = grad[part:]

        @pl.when(depth > 0)
        def _():
            w_hi, w_lo = split2(jnp.transpose(weights_ref[depth]))
            for k in range(5):
                lanes = pl.ds(k * points, points)
                z_hi = zh_ref[:, lanes]
                bar_ref[:, lanes] = dot(w_hi, z_hi) + dot(w_hi, zl_ref[:, lanes]) + dot(w_lo, z_hi)
            fetch_pre(before).wait()

        return carry

    lax.fori_loop(0, layers, layer, 0)
    small = jnp.transpose(cols_ref[...])
    lane = iota((1, width), 1)
    count = jnp.full((1, 1), live_ref[0, 0], jnp.int32).astype(f32)
    last = jnp.where(lane == 0, residual_sum, 0.0) + jnp.where(lane == 1, misfit_sum, 0.0)
    energy = jnp.sum(energy_ref[...], axis=1, keepdims=True)
    last = last + jnp.where(lane == 2, count, 0.0) + jnp.where(lane == 3, energy, 0.0)
    small = jnp.where(iota(small.shape, 0) == small.shape[0] - 1, last, small)
    keep_b_ref[half * width // 2 :, :] = small
    send_b_ref[half * width // 2 :, :] = small


def vmem():
    return pl.BlockSpec(memory_space=pltpu.VMEM)


def smem():
    return pl.BlockSpec(memory_space=pltpu.SMEM)


def hbm():
    return pl.BlockSpec(memory_space=pltpu.HBM)


def call(kernel, name, specs, out_shapes, scratch, flops, limit, outs=None):
    return pl.pallas_call(
        kernel,
        name=name,
        out_shape=out_shapes,
        in_specs=specs,
        out_specs=outs or jax.tree.map(lambda _: vmem(), out_shapes),
        scratch_shapes=scratch,
        compiler_params=pltpu.CompilerParams(vmem_limit_bytes=min(limit << 20, 67043328)),
        cost_estimate=pl.CostEstimate(flops=flops, bytes_accessed=1 << 20, transcendentals=0),
    )


def shape(*dims, dtype=f32):
    return jax.ShapeDtypeStruct(dims, dtype)


def on_device(
    conductivity, owner_rank, tile_slot, offsets, fractions, source, observed, live_count,
    fourier, weights, biases, readout,
):
    devices = lax.axis_size(AXES)
    index = lax.axis_index(AXES)
    points = tile_slot.shape[0]
    tiles = conductivity.shape[0]
    layers, width = biases.shape
    capacity = (2 * points + devices - 1) // devices + 1
    lanes_each = 1 << (capacity - 1).bit_length()
    lanes_each = max(lanes_each, 2 * LANES // devices)
    rows_each = 1 << (-(-11 * lanes_each // LANES) - 1).bit_length()
    slots = devices * lanes_each
    cells = conductivity.size // LANES
    plane = (TILE_SIDE // 4) * tiles
    wide = 5 * points

    live, place = live_count.reshape(1, 1), index.reshape(1, 1)
    owner_row = owner_rank.reshape(1, points)
    source_row = source.reshape(1, points)
    readout_row = readout.reshape(1, width)
    field = conductivity.reshape(tiles, cells // tiles, LANES).transpose(1, 0, 2)
    field = field.reshape(cells, LANES)

    request, outputs, pre, parts = call(
        functools.partial(forward_kernel, devices, layers, tiles, lanes_each),
        "forward",
        [smem()] + [hbm()] * 9,
        (
            shape(devices, rows_each, LANES), shape(8, points),
            shape(layers, width, wide), shape(layers, 2 * width, wide, dtype=bf16),
        ),
        [
            pltpu.VMEM((layers, width, wide), f32),
            pltpu.VMEM((layers + 1, 2 * width, wide), bf16),
            pltpu.VMEM((layers, width, width), f32),
            pltpu.VMEM((width, wide), f32),
            pltpu.VMEM((width, 8), f32),
            pltpu.VMEM((width, 1), f32),
            pltpu.VMEM((1, points), jnp.int32),
            pltpu.VMEM((1, points), jnp.int32),
            pltpu.VMEM((3, points), jnp.int32),
            pltpu.VMEM((3, points), f32),
            pltpu.VMEM((1, points), f32),
            pltpu.VMEM((8, fourier.shape[0]), f32),
            pltpu.VMEM((8, width), f32),
            pltpu.VMEM((3, fourier.shape[0]), f32),
            pltpu.VMEM((layers, width), f32),
            pltpu.VMEM((1, width), f32),
            pltpu.SemaphoreType.DMA((9,)),
            pltpu.SemaphoreType.DMA((2, layers)),
        ],
        6 * 2 * layers * width * width * wide,
        FORWARD_LIMIT,
        outs=(vmem(), vmem(), hbm(), hbm()),
    )(
        live, owner_row, tile_slot.reshape(1, points), offsets, fractions,
        source_row, fourier.T, weights, biases, readout_row,
    )
    received = lax.all_to_all(request, AXES, split_axis=0, concat_axis=0, tiled=True)

    field_here, _ = lax.optimization_barrier((field, outputs))
    window_hi, window_lo, first, last = call(
        functools.partial(prepare_kernel, tiles),
        "prepare",
        [vmem()],
        (
            shape(320, cells, dtype=bf16), shape(320, cells, dtype=bf16),
            shape(TILE_SIDE, tiles, LANES), shape(TILE_SIDE, tiles, LANES),
        ),
        [pltpu.VMEM((cells + 2 * plane, LANES), f32)],
        FILL,
        PREPARE_LIMIT,
    )(field_here)
    up = [(i, i + 1) for i in range(devices - 1)]
    down = [(j, i) for i, j in up]
    before = lax.ppermute(last, AXES, up)
    after = lax.ppermute(first, AXES, down)
    received, before, after = lax.optimization_barrier((received, before, after))

    response, kept = call(
        functools.partial(owner_kernel, devices, tiles, lanes_each),
        "lookup",
        [vmem()] * 3,
        (shape(devices, 1, LANES), shape(16, slots)),
        [pltpu.VMEM((16, slots), f32)],
        2 * 640 * cells * slots,
        LOOKUP_LIMIT,
    )(received, window_hi, window_lo)
    answered = lax.all_to_all(response, AXES, split_axis=0, concat_axis=0, tiled=True)
    grad, energy = call(
        functools.partial(field_kernel, devices, tiles),
        "field",
        [smem()] + [vmem()] * 4,
        (shape(cells, LANES), shape(1, LANES)),
        [
            pltpu.VMEM((cells, slots), bf16),
            pltpu.VMEM((320, slots), bf16),
            pltpu.VMEM((320, slots), bf16),
            pltpu.VMEM((cells + 2 * plane, LANES), f32),
            pltpu.VMEM((cells, 320), f32),
        ],
        FILL,
        SPREAD_LIMIT,
    )(place, kept, field_here, before, after)
    answered, grad = lax.optimization_barrier((answered, grad))

    part_rows = layers * width // 4
    keep_a, keep_b, send_a, send_b = call(
        functools.partial(backward_kernel, devices, layers, lanes_each),
        "backward",
        [smem()] * 2 + [vmem()] * 7 + [hbm()] * 3,
        tuple(shape(rows, width) for rows in (part_rows, part_rows + 8) * 2),
        [
            pltpu.VMEM((layers, width, wide), f32),
            pltpu.VMEM((layers, 2 * width, wide), bf16),
            pltpu.VMEM((layers, width, width), f32),
            pltpu.VMEM((width, wide), f32),
            pltpu.VMEM((width, wide), bf16),
            pltpu.VMEM((width, wide), bf16),
            pltpu.VMEM((width, 1), f32),
            pltpu.VMEM((width, 8), f32),
            pltpu.SemaphoreType.DMA((2, layers + 1)),
        ],
        12 * 2 * layers * width * width * wide,
        BACKWARD_LIMIT,
    )(
        live, place, owner_row, source_row, observed.reshape(1, points),
        answered.reshape(devices, LANES), energy, outputs, readout_row, weights, pre, parts,
    )

    even = [1 << k for k in range(devices.bit_length() - 1)]
    odd = list(even)
    for k in range(1, len(odd) - 1, 2):
        odd[k], odd[k + 1] = odd[k + 1], odd[k]

    def exchange(value, step):
        bits = (even[step], odd[step])
        return lax.ppermute(value, AXES, [(i, i ^ bits[i % 2]) for i in range(devices)])

    def upper_of(step):
        bit = jnp.where(index % 2 == 1, odd[step], even[step])
        return (index & bit) != 0

    main = [keep_a + exchange(send_a, 0), keep_b + exchange(send_b, 0)]
    main[1], extra = main[1][:part_rows], main[1][part_rows:]
    for step in range(1, len(even)):
        half = main[0].shape[0] // 2
        upper = upper_of(step)
        outgoing = [jnp.where(upper, m[:half], m[half:]) for m in main]
        outgoing[1] = jnp.concatenate([outgoing[1], extra], axis=0)
        arrived = [exchange(value, step) for value in outgoing]
        main = [jnp.where(upper, m[half:], m[:half]) + a[:half] for m, a in zip(main, arrived)]
        extra = extra + arrived[1][half:]
    scale = 1.0 / extra[7, 2]
    main = [m * scale for m in main]
    sums = extra[7]
    losses = jnp.stack(
        [sums[0] * scale, sums[1] * scale, sums[3] / (devices * conductivity.size)]
    )
    bias_grad, readout_grad = extra[:layers] * scale, extra[layers] * scale
    for step in reversed(range(len(even))):
        upper = upper_of(step)
        arrived = [exchange(m, step) for m in main]
        main = [
            jnp.concatenate([jnp.where(upper, a, m), jnp.where(upper, m, a)], axis=0)
            for m, a in zip(main, arrived)
        ]
        if step == len(even) - 1:
            main[1], losses, bias_grad, readout_grad = lax.optimization_barrier(
                (main[1], losses, bias_grad, readout_grad)
            )
    weight_grad = jnp.concatenate([m.reshape(layers, width // 2, width) for m in main], axis=1)
    conductivity_grad = grad.reshape(cells // tiles, tiles, LANES).transpose(1, 0, 2)
    return (
        conductivity_grad.reshape(conductivity.shape),
        weight_grad,
        bias_grad,
        readout_grad,
        losses,
    )


def solution(mesh):
    in_specs = (
        P(AXES, None), P(AXES, None), P(AXES), P(None, AXES), P(None, AXES), P(AXES), P(AXES),
        P(AXES), P(), P(), P(), P(),
    )
    out_specs = (P(AXES, None), P(), P(), P(), P())
    return jax.shard_map(
        on_device, mesh=mesh, in_specs=in_specs, out_specs=out_specs, check_vma=False
    )
```

```python
import functools

import jax
import jax.numpy as jnp
from jax import lax
from jax.experimental import pallas as pl
from jax.experimental.pallas import tpu as pltpu
from jax.sharding import PartitionSpec as P

TILE_SIDE = 32
LANES = 128
data_weight = 1.0
smooth_weight = 0.05
AXES = ("gx", "gy")
f32 = jnp.float32
bf16 = jnp.bfloat16
NN = (((1,), (0,)), ((), ()))
NT = (((1,), (1,)), ((), ()))


def dot(a, b, dims=NN):
    return lax.dot_general(a, b, dims, preferred_element_type=f32)


def split2(x):
    hi = x.astype(bf16)
    return hi, (x - hi.astype(f32)).astype(bf16)


def split3(x):
    hi = x.astype(bf16)
    rest = x - hi.astype(f32)
    mid = rest.astype(bf16)
    return hi, mid, (rest - mid.astype(f32)).astype(bf16)


def iota(shape, dim):
    return lax.broadcasted_iota(jnp.int32, shape, dim)


def sin_cos(phase):
    turns = jnp.floor(phase * 0.6366197723675814 + 0.5)
    y = phase - turns * 1.5703125
    y = y - turns * 4.837512969970703125e-4
    y = y - turns * 7.549789954891882e-8
    quarter = turns.astype(jnp.int32)
    y2 = y * y
    s = y + y * y2 * (-1.6666654611e-1 + y2 * (8.3321608736e-3 - y2 * 1.9515295891e-4))
    c = (
        1.0
        - 0.5 * y2
        + y2
        * y2
        * (4.166664568298827e-2 + y2 * (-1.388731625493765e-3 + y2 * 2.443315711809948e-5))
    )
    odd = (quarter & 1) == 1
    sin_part = jnp.where(odd, c, s)
    cos_part = jnp.where(odd, s, c)
    sin_part = jnp.where((quarter & 2) == 2, -sin_part, sin_part)
    cos_part = jnp.where(((quarter + 1) & 2) == 2, -cos_part, cos_part)
    return sin_part, cos_part


def activations(v, z1, z2, z3, z4):
    s = 1.0 - v * v
    q = z1 * z1 + z2 * z2 + z3 * z3
    return s, q, s * z4 - 2.0 * v * s * q


def column_of(row):
    wide = jnp.broadcast_to(row.astype(f32), (8, row.shape[1]))
    return jnp.transpose(wide)[:, 0:1].astype(row.dtype)


def slot_ranks_row(owner_col, owner_row):
    n = owner_row.shape[1]
    same = (owner_col == owner_row) & (iota((n, n), 0) < iota((n, n), 1))
    return jnp.sum(jnp.where(same, 1.0, 0.0), axis=0, keepdims=True).astype(jnp.int32)


def slot_ranks_col(owner_col, owner_row):
    n = owner_row.shape[1]
    same = (owner_col == owner_row) & (iota((n, n), 1) < iota((n, n), 0))
    return jnp.sum(jnp.where(same, 1.0, 0.0), axis=1, keepdims=True).astype(jnp.int32)


FORWARD_ROWS, ROWS = 256, 64
FILL = 4 * 10**9
FORWARD_LIMIT, PREPARE_LIMIT, LOOKUP_LIMIT, SPREAD_LIMIT, BACKWARD_LIMIT = 64, 8, 12, 14, 58


def forward_kernel(
    devices, layers, tiles, lanes_each,
    live_ref, owner_hbm, slot_hbm, offsets_hbm, fractions_hbm, source_hbm,
    fourier_hbm, weights_hbm, biases_hbm, readout_hbm,
    request_ref, outputs_ref, pre_hbm, parts_hbm,
    pre_ref, parts_ref, weights_ref, z_ref, col_ref, bias_ref,
    owner_ref, slot_ref, offsets_ref, fractions_ref, source_ref, fourier_ref, small_ref,
    freq_ref, biases_ref, readout_ref, sems, out_sems,
):
    small_ref[...] = jnp.zeros(small_ref.shape, f32)
    fourier_ref[...] = jnp.zeros(fourier_ref.shape, f32)
    copies = [
        pltpu.make_async_copy(source, target, sems.at[k])
        for k, (source, target) in enumerate(
            (
                (owner_hbm, owner_ref), (slot_hbm, slot_ref), (offsets_hbm, offsets_ref),
                (fractions_hbm, fractions_ref), (fourier_hbm, freq_ref),
                (source_hbm, source_ref), (biases_hbm, biases_ref),
                (readout_hbm, readout_ref), (weights_hbm, weights_ref),
            )
        )
    ]
    for copy in copies:
        copy.start()
    for copy in copies[:-1]:
        copy.wait()
    fourier_ref[0:3, :] = freq_ref[...]
    small_ref[0:layers, :] = biases_ref[...]
    small_ref[layers : layers + 1, :] = readout_ref[...]
    points = slot_ref.shape[1]
    width = weights_ref.shape[1]
    streams = 5
    off = offsets_ref[...]
    fractions = fractions_ref[...]
    owner_row = owner_ref[...]
    slot = slot_ref[...]
    cells = jnp.concatenate(
        [TILE_SIDE * slot + off[0:1], TILE_SIDE * owner_row + off[1:2], off[2:3]], axis=0
    )
    position = cells.astype(f32) + fractions
    f = jnp.transpose(fourier_ref[...])
    phases = f[:, 0:1] * position[0:1] + f[:, 1:2] * position[1:2] + f[:, 2:3] * position[2:3]
    sin_part, cos_part = sin_cos(phases)
    squared = f[:, 0:1] * f[:, 0:1] + f[:, 1:2] * f[:, 1:2] + f[:, 2:3] * f[:, 2:3]
    freqs = f.shape[0]

    def put(stream, top, bottom):
        for start, value in ((0, top), (freqs, bottom)):
            lanes = pl.ds(stream * points, points)
            hi, lo = split2(value)
            parts_ref[0, pl.ds(start, freqs), lanes] = hi
            parts_ref[0, pl.ds(width + start, freqs), lanes] = lo

    put(0, sin_part, cos_part)
    for k in range(3):
        put(k + 1, cos_part * f[:, k : k + 1], -sin_part * f[:, k : k + 1])
    put(4, -sin_part * squared, -cos_part * squared)

    small_cols = jnp.transpose(small_ref[...])
    col_ref[...] = small_cols
    copies[-1].wait()

    def leave_parts(depth):
        return pltpu.make_async_copy(
            parts_ref.at[depth], parts_hbm.at[depth], out_sems.at[0, depth]
        )

    def leave_pre(depth):
        return pltpu.make_async_copy(pre_ref.at[depth], pre_hbm.at[depth], out_sems.at[1, depth])

    def layer(depth, carry):
        leave_parts(depth).start()
        w_hi, w_lo = split2(weights_ref[depth])
        for k in range(streams):
            lanes = pl.ds(k * points, points)
            h_hi = parts_ref[depth, 0:width, lanes]
            h_lo = parts_ref[depth, width:, lanes]
            z_ref[:, lanes] = dot(w_hi, h_hi) + dot(w_hi, h_lo) + dot(w_lo, h_hi)
        bias = jnp.sum(
            jnp.where(iota(small_cols.shape, 1) == depth, small_cols, 0.0), axis=1, keepdims=True
        )
        bias_ref[...] = bias

        def chunk(c, inner):
            rows = pl.ds(pl.multiple_of(c * FORWARD_ROWS, FORWARD_ROWS), FORWARD_ROWS)
            low_rows = pl.ds(pl.multiple_of(width + c * FORWARD_ROWS, FORWARD_ROWS), FORWARD_ROWS)

            def z_of(k):
                return z_ref[rows, pl.ds(k * points, points)]

            v = jnp.tanh(z_of(0) + bias_ref[rows, :])
            z1, z2, z3, z4 = z_of(1), z_of(2), z_of(3), z_of(4)
            s, _, curve = activations(v, z1, z2, z3, z4)
            for k, (kept, h) in enumerate(
                ((v, v), (z1, s * z1), (z2, s * z2), (z3, s * z3), (z4, curve))
            ):
                lanes = pl.ds(k * points, points)
                pre_ref[depth, rows, lanes] = kept
                hi, lo = split2(h)
                parts_ref[depth + 1, rows, lanes] = hi
                parts_ref[depth + 1, low_rows, lanes] = lo
            return inner

        lax.fori_loop(0, width // FORWARD_ROWS, chunk, 0)
        leave_pre(depth).start()
        return carry

    lax.fori_loop(0, layers, layer, 0)

    def readout_chunk(c, totals):
        rows = pl.ds(pl.multiple_of(c * FORWARD_ROWS, FORWARD_ROWS), FORWARD_ROWS)
        v, z1, z2, z3, z4 = [
            pre_ref[layers - 1, rows, pl.ds(k * points, points)] for k in range(streams)
        ]
        s, _, curve = activations(v, z1, z2, z3, z4)
        r = col_ref[rows, layers : layers + 1]
        hs = (v, s * z1, s * z2, s * z3, curve)
        return tuple(t + jnp.sum(r * h, axis=0, keepdims=True) for t, h in zip(totals, hs))

    zero = tuple(jnp.zeros((1, points), f32) for _ in range(streams))
    out = lax.fori_loop(0, width // FORWARD_ROWS, readout_chunk, zero)
    outputs = jnp.concatenate(list(out) + [jnp.zeros((3, points), f32)], axis=0)
    outputs_ref[...] = outputs

    live = jnp.where(iota((1, points), 1) < live_ref[0, 0], 1.0, 0.0)
    row_index = ((off[0:1] * (TILE_SIDE // 4) + off[1:2] // 4) * tiles + slot).astype(f32)
    lane_index = ((off[1:2] % 4) * TILE_SIDE + off[2:3]).astype(f32)
    comps = [
        row_index, lane_index, fractions[0:1], fractions[1:2], fractions[2:3],
        outputs[1:2], outputs[2:3], outputs[3:4], outputs[4:5], source_ref[...], live,
    ]
    to_owner = owner_row == iota((devices, points), 0)
    ranks = slot_ranks_col(column_of(owner_row), owner_row)
    place = jnp.where(ranks == iota((points, LANES), 1), 1.0, 0.0).astype(bf16)
    spread = jnp.concatenate([jnp.where(to_owner, c, 0.0) for c in comps], axis=0)
    a, b, c = split3(spread)
    packed = dot(a, place) + dot(b, place) + dot(c, place)
    rows_each, lane_groups = request_ref.shape[1], LANES // lanes_each
    for j in range(rows_each):
        total = jnp.zeros((devices, LANES), f32)
        for m in range(lane_groups):
            k = rows_each * m + j
            if k < len(comps):
                part = packed[k * devices : (k + 1) * devices]
                total = total + (pltpu.roll(part, lanes_each * m, 1) if m else part)
        request_ref[:, j, :] = total
    for depth in range(layers):
        leave_parts(depth).wait()
        leave_pre(depth).wait()


def owner_kernel(
    devices, tiles, lanes_each,
    received_ref, window_hi, window_lo,
    response_ref, kept_ref,
    x_ref,
):
    cells = window_hi.shape[1]
    group = LANES // lanes_each
    blocks = devices // group
    slots = blocks * LANES
    rows_each = received_ref.shape[1]
    lane_block = iota((rows_each * group, LANES), 1) // lanes_each
    for j in range(blocks):
        total = None
        for g in range(group):
            part = received_ref[group * j + g]
            moved = jnp.concatenate(
                [
                    pltpu.roll(part, lanes_each * ((g - m) % group), 1) if g != m else part
                    for m in range(group)
                ],
                axis=0,
            )
            total = moved if total is None else jnp.where(lane_block == g, moved, total)
        x_ref[:, j * LANES : (j + 1) * LANES] = total

    step = 2 * LANES
    for start in range(0, slots, step):
        x = x_ref[:, start : start + step]
        rows = x[0:1].astype(jnp.int32)
        place = x[1:2].astype(jnp.int32)
        hot = jnp.where(iota((cells, step), 0) == rows, 1.0, 0.0).astype(bf16)
        found = dot(window_hi[...], hot) + dot(window_lo[...], hot)
        y_mod = place // TILE_SIDE
        z_cell = place % TILE_SIDE
        z_iota = iota((TILE_SIDE, step), 0)
        at_z = (z_iota == z_cell, z_iota == z_cell + 1)
        corner = {}
        for a in range(2):
            parts = [found[a * 160 + TILE_SIDE * j : a * 160 + TILE_SIDE * (j + 1)] for j in range(5)]
            for b in range(2):
                rows_y = jnp.where(y_mod == 0, parts[b], 0.0)
                for j in range(1, 4):
                    rows_y = jnp.where(y_mod == j, parts[j + b], rows_y)
                for c in range(2):
                    corner[a, b, c] = jnp.sum(
                        jnp.where(at_z[c], rows_y, 0.0), axis=0, keepdims=True
                    )
        fr = [x[2:3], x[3:4], x[4:5]]
        w = [(1.0 - t, t) for t in fr]
        sign = (-1.0, 1.0)
        values = [jnp.zeros((1, step), f32) for _ in range(4)]
        for (a, b, c), k in corner.items():
            values[0] = values[0] + w[0][a] * w[1][b] * w[2][c] * k
            values[1] = values[1] + sign[a] * w[1][b] * w[2][c] * k
            values[2] = values[2] + w[0][a] * sign[b] * w[2][c] * k
            values[3] = values[3] + w[0][a] * w[1][b] * sign[c] * k
        du = [x[5:6], x[6:7], x[7:8]]
        lap = x[8:9]
        residual = (
            -(values[0] * lap + (values[1] * du[0] + values[2] * du[1] + values[3] * du[2]))
            - x[9:10]
        )
        scaled = 2.0 * x[10:11] * residual
        zeros = jnp.zeros((4, step), f32)
        answer = jnp.concatenate(values + [zeros], axis=0)
        sub = iota((8, LANES), 0)
        lane_of = iota((8, LANES), 1) // lanes_each
        for j in range(step // LANES):
            block = start // LANES + j
            part = answer[:, j * LANES : (j + 1) * LANES]
            turned = [pltpu.roll(part, lanes_each * k, 1) if k else part for k in range(group)]
            for g in range(group):
                picked = jnp.zeros((8, LANES), f32)
                for c in range(4):
                    picked = jnp.where((sub == c) & (lane_of == c), turned[(c - g) % group], picked)
                response_ref[group * block + g] = jnp.sum(picked, axis=0, keepdims=True)
        kept_ref[:, start : start + step] = jnp.concatenate(
            [x[0:5], -scaled * lap, -scaled * du[0], -scaled * du[1], -scaled * du[2]]
            + [jnp.zeros((7, step), f32)],
            axis=0,
        )


def field_kernel(
    devices, tiles,
    index_ref, kept_ref, field_ref, before_ref, after_ref,
    grad_ref, energy_ref,
    hot_ref, c_hi, c_lo, sum_ref, part_ref,
):
    cells = field_ref.shape[0]
    slots = kept_ref.shape[1]
    plane = (TILE_SIDE // 4) * tiles
    step = 2 * LANES
    for start in range(0, slots, step):
        lanes = slice(start, start + step)
        x = kept_ref[:, lanes]
        rows = x[0:1].astype(jnp.int32)
        place = x[1:2].astype(jnp.int32)
        hot_ref[:, lanes] = jnp.where(iota((cells, step), 0) == rows, 1.0, 0.0).astype(bf16)
        y_mod = place // TILE_SIDE
        z_cell = place % TILE_SIDE
        z_iota = iota((TILE_SIDE, step), 0)
        at_z = (z_iota == z_cell, z_iota == z_cell + 1)
        w = [(1.0 - x[k : k + 1], x[k : k + 1]) for k in (2, 3, 4)]
        g = [x[k : k + 1] for k in (5, 6, 7, 8)]
        sign = (-1.0, 1.0)
        for a in range(2):
            along = []
            for b in range(2):
                pair = []
                for c in range(2):
                    pair.append(
                        g[0] * w[0][a] * w[1][b] * w[2][c]
                        + g[1] * sign[a] * w[1][b] * w[2][c]
                        + g[2] * w[0][a] * sign[b] * w[2][c]
                        + g[3] * w[0][a] * w[1][b] * sign[c]
                    )
                along.append(jnp.where(at_z[0], pair[0], 0.0) + jnp.where(at_z[1], pair[1], 0.0))
            for j in range(5):
                value = jnp.where(y_mod == j, along[0], 0.0) + jnp.where(
                    y_mod == j - 1, along[1], 0.0
                )
                hi, lo = split2(value)
                at = a * 128 + TILE_SIDE * j if j < 4 else 256 + a * TILE_SIDE
                c_hi[at : at + TILE_SIDE, lanes] = hi
                c_lo[at : at + TILE_SIDE, lanes] = lo
    sum_ref[...] = jnp.zeros(sum_ref.shape, f32)
    block = 2 * LANES
    for start in range(0, cells, block):
        hot = hot_ref[start : start + block, :]
        part = dot(hot, c_hi[...], NT) + dot(hot, c_lo[...], NT)
        part_ref[start : start + block, :] = part
    sum_ref[0:cells, :] = part_ref[:, 0:128]
    sum_ref[plane : plane + cells, :] += part_ref[:, 128:256]
    low = slice(0, TILE_SIDE)
    sum_ref[tiles : tiles + cells, low] += part_ref[:, 256 : 256 + TILE_SIDE]
    sum_ref[plane + tiles : plane + tiles + cells, low] += part_ref[
        :, 256 + TILE_SIDE : 256 + 2 * TILE_SIDE
    ]

    me = index_ref[0, 0]
    row = iota((plane, LANES), 0)
    lane = iota((plane, LANES), 1)
    z_inner = (lane % TILE_SIDE) < TILE_SIDE - 1
    first_row = row < tiles
    last_row = row >= plane - tiles
    low_lane = lane < TILE_SIDE
    high_lane = lane >= LANES - TILE_SIDE
    has_after = jnp.where(me < devices - 1, 1.0, 0.0)
    has_before = jnp.where(me > 0, 1.0, 0.0)
    after_mask = jnp.where(last_row & high_lane, has_after, 1.0)
    before_mask = jnp.where(first_row & low_lane, has_before, 1.0)
    next_tile = (row % tiles) < tiles - 1
    prev_tile = (row % tiles) > 0

    def load(x):
        return field_ref[pl.ds(pl.multiple_of(x * plane, plane), plane), :]

    def plane_step(x, energy):
        here = load(x)
        diff_z = jnp.where(z_inner, pltpu.roll(here, LANES - 1, 1) - here, 0.0)
        grad = pltpu.roll(diff_z, 1, 1) - diff_z
        energy = energy + diff_z * diff_z
        above = jnp.concatenate([here[tiles:], after_ref[x]], axis=0)
        up = pltpu.roll(jnp.where(low_lane, above, here), LANES - TILE_SIDE, 1)
        below = jnp.concatenate([before_ref[x], here[: plane - tiles]], axis=0)
        down = pltpu.roll(jnp.where(high_lane, below, here), TILE_SIDE, 1)
        diff_up = (up - here) * after_mask
        diff_down = (here - down) * before_mask
        grad = grad + diff_down - diff_up
        energy = energy + diff_down * diff_down
        first = x == 0
        last = x == TILE_SIDE - 1
        nxt = load(jnp.where(last, 0, x + 1))
        nxt = jnp.where(last, pltpu.roll(nxt, plane - 1, 0), nxt)
        prv = load(jnp.where(first, TILE_SIDE - 1, x - 1))
        prv = jnp.where(first, pltpu.roll(prv, 1, 0), prv)
        diff_next = jnp.where(jnp.logical_not(last) | next_tile, nxt - here, 0.0)
        diff_prev = jnp.where(jnp.logical_not(first) | prev_tile, here - prv, 0.0)
        grad = grad + diff_prev - diff_next
        energy = energy + diff_prev * diff_prev
        at = pl.ds(pl.multiple_of(x * plane, plane), plane)
        grad_ref[at, :] = sum_ref[at, :] + 2.0 * smooth_weight * grad
        return energy

    energy = lax.fori_loop(
        0, TILE_SIDE, plane_step, jnp.zeros((plane, LANES), f32), unroll=4
    )
    energy_ref[...] = jnp.sum(energy, axis=0, keepdims=True)


def prepare_kernel(
    tiles,
    field_ref,
    window_hi, window_lo, first_ref, last_ref,
    padded_ref,
):
    cells = field_ref.shape[0]
    plane = (TILE_SIDE // 4) * tiles
    for x in range(TILE_SIDE):
        first_ref[x] = field_ref[x * plane : x * plane + tiles, :]
        last_ref[x] = field_ref[(x + 1) * plane - tiles : (x + 1) * plane, :]
    padded_ref[0:cells, :] = field_ref[...]
    padded_ref[cells:, :] = jnp.zeros((padded_ref.shape[0] - cells, LANES), f32)
    for a in range(2):
        base = a * plane
        main = jnp.transpose(padded_ref[base : base + cells, :])
        hi, lo = split2(main)
        window_hi[a * 160 : a * 160 + 128, :] = hi
        window_lo[a * 160 : a * 160 + 128, :] = lo
        extra = jnp.transpose(padded_ref[base + tiles : base + tiles + cells, :])[0:TILE_SIDE]
        hi, lo = split2(extra)
        window_hi[a * 160 + 128 : a * 160 + 160, :] = hi
        window_lo[a * 160 + 128 : a * 160 + 160, :] = lo


def backward_kernel(
    devices, layers, lanes_each,
    live_ref, index_ref, owner_row_ref, source_ref, observed_ref, response_ref, energy_ref,
    outputs_ref, readout_ref, weights_hbm, pre_hbm, parts_hbm,
    keep_a_ref, keep_b_ref, send_a_ref, send_b_ref,
    pre_ref, parts_ref, weights_ref, bar_ref, zh_ref, zl_ref, col_ref, cols_ref, sems,
):
    def fetch_pre(k):
        return pltpu.make_async_copy(pre_hbm.at[k], pre_ref.at[k], sems.at[0, k])

    def fetch_parts(k):
        return pltpu.make_async_copy(parts_hbm.at[k], parts_ref.at[k], sems.at[1, k])

    weight_copy = pltpu.make_async_copy(weights_hbm, weights_ref, sems.at[0, layers])
    fetch_pre(layers - 1).start()
    weight_copy.start()
    fetch_parts(layers - 1).start()
    points = owner_row_ref.shape[1]
    width = weights_hbm.shape[1]
    owner_row = owner_row_ref[...]
    ranks = slot_ranks_row(column_of(owner_row), owner_row)
    picked = jnp.where(ranks == iota((lanes_each, points), 0), 1.0, 0.0)
    from_owner = jnp.where(owner_row == iota((devices, points), 0), 1.0, 0.0).astype(bf16)
    a, b, c = split3(jnp.transpose(response_ref[...])[0 : 4 * lanes_each])
    wide = dot(a, from_owner) + dot(b, from_owner) + dot(c, from_owner)
    values = [
        jnp.sum(picked * wide[k * lanes_each : (k + 1) * lanes_each], axis=0, keepdims=True)
        for k in range(4)
    ]
    outputs = outputs_ref[...]
    out = [outputs[k : k + 1] for k in range(5)]
    live = jnp.where(iota((1, points), 1) < live_ref[0, 0], 1.0, 0.0)
    misfit = out[0] - observed_ref[...]
    residual = (
        -(values[0] * out[4] + (values[1] * out[1] + values[2] * out[2] + values[3] * out[3]))
        - source_ref[...]
    )
    scaled = 2.0 * live * residual
    out_grad = [2.0 * data_weight * live * misfit] + [-scaled * values[k] for k in (1, 2, 3, 0)]
    residual_sum = jnp.sum(live * residual * residual, axis=1, keepdims=True)
    misfit_sum = jnp.sum(live * misfit * misfit, axis=1, keepdims=True)
    col_ref[...] = column_of(readout_ref[...])
    cols_ref[...] = jnp.zeros(cols_ref.shape, f32)
    lane8 = iota((ROWS, cols_ref.shape[1]), 1)
    chunks = width // ROWS

    def rows_of(c):
        return pl.ds(pl.multiple_of(c * ROWS, ROWS), ROWS)

    def pre_of(depth, rows):
        return [pre_ref[depth, rows, pl.ds(k * points, points)] for k in range(5)]

    def readout_chunk(c, carry):
        rows = rows_of(c)
        v, z1, z2, z3, z4 = pre_of(layers - 1, rows)
        s, _, curve = activations(v, z1, z2, z3, z4)
        total = out_grad[0] * v + out_grad[1] * (s * z1) + out_grad[2] * (s * z2)
        total = total + out_grad[3] * (s * z3) + out_grad[4] * curve
        grad = jnp.sum(total, axis=1, keepdims=True)
        cols_ref[rows, :] += jnp.where(lane8 == layers, grad, 0.0)
        r = col_ref[rows, :]
        for k in range(5):
            bar_ref[rows, pl.ds(k * points, points)] = r * out_grad[k]
        return carry

    fetch_pre(layers - 1).wait()
    lax.fori_loop(0, chunks, readout_chunk, 0)
    weight_copy.wait()
    mine = index_ref[0, 0] % 2
    half = layers // 2

    def layer(step, carry):
        depth = layers - 1 - step
        before = jnp.maximum(depth - 1, 0)

        @pl.when(depth > 0)
        def _():
            fetch_pre(before).start()
            fetch_parts(before).start()

        def bars(c, inner):
            rows = rows_of(c)
            v, z1, z2, z3, z4 = pre_of(depth, rows)
            b = [bar_ref[rows, pl.ds(k * points, points)] for k in range(5)]
            s = 1.0 - v * v
            q = z1 * z1 + z2 * z2 + z3 * z3
            slope = b[1] * z1 + b[2] * z2 + b[3] * z3
            v4c = 4.0 * v * b[4]
            z_bar = [
                s
                * (
                    b[0]
                    - 2.0 * v * slope
                    + b[4] * (q * (4.0 * v * v - 2.0 * s) - 2.0 * v * z4)
                ),
                s * (b[1] - v4c * z1),
                s * (b[2] - v4c * z2),
                s * (b[3] - v4c * z3),
                s * b[4],
            ]
            grad = jnp.sum(z_bar[0], axis=1, keepdims=True)
            cols_ref[rows, :] += jnp.where(lane8 == depth, grad, 0.0)
            for k in range(5):
                lanes = pl.ds(k * points, points)
                hi, lo = split2(z_bar[k])
                zh_ref[rows, lanes] = hi
                zl_ref[rows, lanes] = lo
            return inner

        lax.fori_loop(0, chunks, bars, 0, unroll=2)
        fetch_parts(depth).wait()
        h_hi, h_lo = parts_ref[depth, 0:width], parts_ref[depth, width:]
        z_hi, z_lo = zh_ref[...], zl_ref[...]
        grad = dot(z_hi, h_hi, NT) + dot(z_hi, h_lo, NT) + dot(z_lo, h_hi, NT)
        upper = (depth >= half).astype(jnp.int32)
        part = width // 2
        at = pl.ds(pl.multiple_of((depth - upper * half) * part, part), part)

        @pl.when(mine == upper)
        def _():
            keep_a_ref[at, :] = grad[:part]
            keep_b_ref[at, :] = grad[part:]

        @pl.when(mine != upper)
        def _():
            send_a_ref[at, :] = grad[:part]
            send_b_ref[at, :] = grad[part:]

        @pl.when(depth > 0)
        def _():
            w_hi, w_lo = split2(jnp.transpose(weights_ref[depth]))
            for k in range(5):
                lanes = pl.ds(k * points, points)
                z_hi = zh_ref[:, lanes]
                bar_ref[:, lanes] = dot(w_hi, z_hi) + dot(w_hi, zl_ref[:, lanes]) + dot(w_lo, z_hi)
            fetch_pre(before).wait()

        return carry

    lax.fori_loop(0, layers, layer, 0)
    small = jnp.transpose(cols_ref[...])
    lane = iota((1, width), 1)
    count = jnp.full((1, 1), live_ref[0, 0], jnp.int32).astype(f32)
    last = jnp.where(lane == 0, residual_sum, 0.0) + jnp.where(lane == 1, misfit_sum, 0.0)
    energy = jnp.sum(energy_ref[...], axis=1, keepdims=True)
    last = last + jnp.where(lane == 2, count, 0.0) + jnp.where(lane == 3, energy, 0.0)
    small = jnp.where(iota(small.shape, 0) == small.shape[0] - 1, last, small)
    keep_b_ref[half * width // 2 :, :] = small
    send_b_ref[half * width // 2 :, :] = small


def finish_kernel(cells_total, sums_ref, bias_ref, readout_ref, losses_ref, scale_ref):
    layers = bias_ref.shape[0]
    width = bias_ref.shape[1]
    sums = sums_ref[...]
    lane = iota((1, width), 1)
    last = sums[7:8]
    count = jnp.sum(jnp.where(lane == 2, last, 0.0), axis=1, keepdims=True)
    scale = jnp.broadcast_to(1.0 / count, (1, width))
    bias_ref[...] = sums[:layers] * scale
    readout_ref[...] = sums[layers : layers + 1] * scale
    energy = jnp.sum(jnp.where(lane == 3, last, 0.0), axis=1, keepdims=True)
    losses = jnp.where(lane == 2, energy / cells_total, last * scale)
    losses_ref[...] = losses[:, 0:3]
    scale_ref[...] = scale


def vmem():
    return pl.BlockSpec(memory_space=pltpu.VMEM)


def smem():
    return pl.BlockSpec(memory_space=pltpu.SMEM)


def hbm():
    return pl.BlockSpec(memory_space=pltpu.HBM)


def call(kernel, name, specs, out_shapes, scratch, flops, limit, outs=None):
    return pl.pallas_call(
        kernel,
        name=name,
        out_shape=out_shapes,
        in_specs=specs,
        out_specs=outs or jax.tree.map(lambda _: vmem(), out_shapes),
        scratch_shapes=scratch,
        compiler_params=pltpu.CompilerParams(vmem_limit_bytes=min(limit << 20, 67043328)),
        cost_estimate=pl.CostEstimate(flops=flops, bytes_accessed=1 << 20, transcendentals=0),
    )


def shape(*dims, dtype=f32):
    return jax.ShapeDtypeStruct(dims, dtype)


def on_device(
    conductivity, owner_rank, tile_slot, offsets, fractions, source, observed, live_count,
    fourier, weights, biases, readout,
):
    devices = lax.axis_size(AXES)
    index = lax.axis_index(AXES)
    points = tile_slot.shape[0]
    tiles = conductivity.shape[0]
    layers, width = biases.shape
    capacity = (2 * points + devices - 1) // devices + 1
    lanes_each = 1 << (capacity - 1).bit_length()
    lanes_each = max(lanes_each, 2 * LANES // devices)
    rows_each = 1 << (-(-11 * lanes_each // LANES) - 1).bit_length()
    slots = devices * lanes_each
    cells = conductivity.size // LANES
    plane = (TILE_SIDE // 4) * tiles
    wide = 5 * points

    live, place = live_count.reshape(1, 1), index.reshape(1, 1)
    owner_row = owner_rank.reshape(1, points)
    source_row = source.reshape(1, points)
    readout_row = readout.reshape(1, width)
    field = conductivity.reshape(tiles, cells // tiles, LANES).transpose(1, 0, 2)
    field = field.reshape(cells, LANES)

    request, outputs, pre, parts = call(
        functools.partial(forward_kernel, devices, layers, tiles, lanes_each),
        "forward",
        [smem()] + [hbm()] * 9,
        (
            shape(devices, rows_each, LANES), shape(8, points),
            shape(layers, width, wide), shape(layers, 2 * width, wide, dtype=bf16),
        ),
        [
            pltpu.VMEM((layers, width, wide), f32),
            pltpu.VMEM((layers + 1, 2 * width, wide), bf16),
            pltpu.VMEM((layers, width, width), f32),
            pltpu.VMEM((width, wide), f32),
            pltpu.VMEM((width, 8), f32),
            pltpu.VMEM((width, 1), f32),
            pltpu.VMEM((1, points), jnp.int32),
            pltpu.VMEM((1, points), jnp.int32),
            pltpu.VMEM((3, points), jnp.int32),
            pltpu.VMEM((3, points), f32),
            pltpu.VMEM((1, points), f32),
            pltpu.VMEM((8, fourier.shape[0]), f32),
            pltpu.VMEM((8, width), f32),
            pltpu.VMEM((3, fourier.shape[0]), f32),
            pltpu.VMEM((layers, width), f32),
            pltpu.VMEM((1, width), f32),
            pltpu.SemaphoreType.DMA((9,)),
            pltpu.SemaphoreType.DMA((2, layers)),
        ],
        6 * 2 * layers * width * width * wide,
        FORWARD_LIMIT,
        outs=(vmem(), vmem(), hbm(), hbm()),
    )(
        live, owner_row, tile_slot.reshape(1, points), offsets, fractions,
        source_row, fourier.T, weights, biases, readout_row,
    )
    received = lax.all_to_all(request, AXES, split_axis=0, concat_axis=0, tiled=True)

    field_here, _ = lax.optimization_barrier((field, outputs))
    window_hi, window_lo, first, last = call(
        functools.partial(prepare_kernel, tiles),
        "prepare",
        [vmem()],
        (
            shape(320, cells, dtype=bf16), shape(320, cells, dtype=bf16),
            shape(TILE_SIDE, tiles, LANES), shape(TILE_SIDE, tiles, LANES),
        ),
        [pltpu.VMEM((cells + 2 * plane, LANES), f32)],
        FILL,
        PREPARE_LIMIT,
    )(field_here)
    up = [(i, i + 1) for i in range(devices - 1)]
    down = [(j, i) for i, j in up]
    before = lax.ppermute(last, AXES, up)
    after = lax.ppermute(first, AXES, down)
    received, before, after = lax.optimization_barrier((received, before, after))

    response, kept = call(
        functools.partial(owner_kernel, devices, tiles, lanes_each),
        "lookup",
        [vmem()] * 3,
        (shape(devices, 1, LANES), shape(16, slots)),
        [pltpu.VMEM((16, slots), f32)],
        2 * 640 * cells * slots,
        LOOKUP_LIMIT,
    )(received, window_hi, window_lo)
    answered = lax.all_to_all(response, AXES, split_axis=0, concat_axis=0, tiled=True)
    grad, energy = call(
        functools.partial(field_kernel, devices, tiles),
        "field",
        [smem()] + [vmem()] * 4,
        (shape(cells, LANES), shape(1, LANES)),
        [
            pltpu.VMEM((cells, slots), bf16),
            pltpu.VMEM((320, slots), bf16),
            pltpu.VMEM((320, slots), bf16),
            pltpu.VMEM((cells + 2 * plane, LANES), f32),
            pltpu.VMEM((cells, 320), f32),
        ],
        FILL,
        SPREAD_LIMIT,
    )(place, kept, field_here, before, after)
    answered, grad = lax.optimization_barrier((answered, grad))

    part_rows = layers * width // 4
    keep_a, keep_b, send_a, send_b = call(
        functools.partial(backward_kernel, devices, layers, lanes_each),
        "backward",
        [smem()] * 2 + [vmem()] * 7 + [hbm()] * 3,
        tuple(shape(rows, width) for rows in (part_rows, part_rows + 8) * 2),
        [
            pltpu.VMEM((layers, width, wide), f32),
            pltpu.VMEM((layers, 2 * width, wide), bf16),
            pltpu.VMEM((layers, width, width), f32),
            pltpu.VMEM((width, wide), f32),
            pltpu.VMEM((width, wide), bf16),
            pltpu.VMEM((width, wide), bf16),
            pltpu.VMEM((width, 1), f32),
            pltpu.VMEM((width, 8), f32),
            pltpu.SemaphoreType.DMA((2, layers + 1)),
        ],
        12 * 2 * layers * width * width * wide,
        BACKWARD_LIMIT,
    )(
        live, place, owner_row, source_row, observed.reshape(1, points),
        answered.reshape(devices, LANES), energy, outputs, readout_row, weights, pre, parts,
    )

    even = [1 << k for k in range(devices.bit_length() - 1)]
    odd = list(even)
    for k in range(1, len(odd) - 1, 2):
        odd[k], odd[k + 1] = odd[k + 1], odd[k]

    def exchange(value, step):
        bits = (even[step], odd[step])
        return lax.ppermute(value, AXES, [(i, i ^ bits[i % 2]) for i in range(devices)])

    def upper_of(step):
        bit = jnp.where(index % 2 == 1, odd[step], even[step])
        return (index & bit) != 0

    main = [keep_a + exchange(send_a, 0), keep_b + exchange(send_b, 0)]
    main[1], extra = main[1][:part_rows], main[1][part_rows:]
    for step in range(1, len(even)):
        half = main[0].shape[0] // 2
        upper = upper_of(step)
        outgoing = [jnp.where(upper, m[:half], m[half:]) for m in main]
        outgoing[1] = jnp.concatenate([outgoing[1], extra], axis=0)
        arrived = [exchange(value, step) for value in outgoing]
        main = [jnp.where(upper, m[half:], m[:half]) + a[:half] for m, a in zip(main, arrived)]
        extra = extra + arrived[1][half:]
    for step in reversed(range(len(even))):
        upper = upper_of(step)
        outgoing = list(main)
        if step == len(even) - 1:
            outgoing[1] = jnp.concatenate([main[1], extra], axis=0)
        arrived = [exchange(value, step) for value in outgoing]
        if step == len(even) - 1:
            rows = main[1].shape[0]
            arrived[1], extra = arrived[1][:rows], arrived[1][rows:]
        main = [
            jnp.concatenate([jnp.where(upper, a, m), jnp.where(upper, m, a)], axis=0)
            for m, a in zip(main, arrived)
        ]
    bias_grad, readout_grad, losses, scale = call(
        functools.partial(finish_kernel, float(devices * conductivity.size)),
        "finish",
        [vmem()],
        (shape(layers, width), shape(1, width), shape(1, 3), shape(1, width)),
        [],
        FILL,
        4,
    )(extra)
    weight_grad = scale * jnp.concatenate(
        [m.reshape(layers, width // 2, width) for m in main], axis=1
    )
    conductivity_grad = grad.reshape(cells // tiles, tiles, LANES).transpose(1, 0, 2)
    return (
        conductivity_grad.reshape(conductivity.shape),
        weight_grad,
        bias_grad,
        readout_grad.reshape(readout.shape),
        losses.reshape(3),
    )


def solution(mesh):
    in_specs = (
        P(AXES, None), P(AXES, None), P(AXES), P(None, AXES), P(None, AXES), P(AXES), P(AXES),
        P(AXES), P(), P(), P(), P(),
    )
    out_specs = (P(AXES, None), P(), P(), P(), P())
    return jax.shard_map(
        on_device, mesh=mesh, in_specs=in_specs, out_specs=out_specs, check_vma=False
    )
```

```python
import functools

import jax
import jax.numpy as jnp
from jax import lax
from jax.experimental import pallas as pl
from jax.experimental.pallas import tpu as pltpu
from jax.sharding import PartitionSpec as P

TILE_SIDE = 32
LANES = 128
data_weight = 1.0
smooth_weight = 0.05
AXES = ("gx", "gy")
f32 = jnp.float32
bf16 = jnp.bfloat16
NN = (((1,), (0,)), ((), ()))
NT = (((1,), (1,)), ((), ()))


def dot(a, b, dims=NN):
    return lax.dot_general(a, b, dims, preferred_element_type=f32)


def split2(x):
    hi = x.astype(bf16)
    return hi, (x - hi.astype(f32)).astype(bf16)


def split3(x):
    hi = x.astype(bf16)
    rest = x - hi.astype(f32)
    mid = rest.astype(bf16)
    return hi, mid, (rest - mid.astype(f32)).astype(bf16)


def iota(shape, dim):
    return lax.broadcasted_iota(jnp.int32, shape, dim)


def sin_cos(phase):
    turns = jnp.floor(phase * 0.6366197723675814 + 0.5)
    y = phase - turns * 1.5703125
    y = y - turns * 4.837512969970703125e-4
    y = y - turns * 7.549789954891882e-8
    quarter = turns.astype(jnp.int32)
    y2 = y * y
    s = y + y * y2 * (-1.6666654611e-1 + y2 * (8.3321608736e-3 - y2 * 1.9515295891e-4))
    c = (
        1.0
        - 0.5 * y2
        + y2
        * y2
        * (4.166664568298827e-2 + y2 * (-1.388731625493765e-3 + y2 * 2.443315711809948e-5))
    )
    odd = (quarter & 1) == 1
    sin_part = jnp.where(odd, c, s)
    cos_part = jnp.where(odd, s, c)
    sin_part = jnp.where((quarter & 2) == 2, -sin_part, sin_part)
    cos_part = jnp.where(((quarter + 1) & 2) == 2, -cos_part, cos_part)
    return sin_part, cos_part


def activations(v, z1, z2, z3, z4):
    s = 1.0 - v * v
    q = z1 * z1 + z2 * z2 + z3 * z3
    return s, q, s * z4 - 2.0 * v * s * q


def column_of(row):
    wide = jnp.broadcast_to(row.astype(f32), (8, row.shape[1]))
    return jnp.transpose(wide)[:, 0:1].astype(row.dtype)


def slot_ranks_row(owner_col, owner_row):
    n = owner_row.shape[1]
    same = (owner_col == owner_row) & (iota((n, n), 0) < iota((n, n), 1))
    return jnp.sum(jnp.where(same, 1.0, 0.0), axis=0, keepdims=True).astype(jnp.int32)


def slot_ranks_col(owner_col, owner_row):
    n = owner_row.shape[1]
    same = (owner_col == owner_row) & (iota((n, n), 1) < iota((n, n), 0))
    return jnp.sum(jnp.where(same, 1.0, 0.0), axis=1, keepdims=True).astype(jnp.int32)


FORWARD_ROWS, ROWS = 256, 64
FILL = 4 * 10**9
FORWARD_LIMIT, PREPARE_LIMIT, LOOKUP_LIMIT, SPREAD_LIMIT, BACKWARD_LIMIT = 64, 8, 12, 14, 48


def forward_kernel(
    devices, layers, tiles, lanes_each,
    live_ref, owner_hbm, slot_hbm, offsets_hbm, fractions_hbm, source_hbm,
    fourier_hbm, weights_hbm, biases_hbm, readout_hbm,
    request_ref, outputs_ref, pre_hbm, parts_hbm,
    pre_ref, parts_ref, weights_ref, z_ref, col_ref, bias_ref,
    owner_ref, slot_ref, offsets_ref, fractions_ref, source_ref, fourier_ref, small_ref,
    freq_ref, biases_ref, readout_ref, sems, out_sems,
):
    small_ref[...] = jnp.zeros(small_ref.shape, f32)
    fourier_ref[...] = jnp.zeros(fourier_ref.shape, f32)
    copies = [
        pltpu.make_async_copy(source, target, sems.at[k])
        for k, (source, target) in enumerate(
            (
                (owner_hbm, owner_ref), (slot_hbm, slot_ref), (offsets_hbm, offsets_ref),
                (fractions_hbm, fractions_ref), (fourier_hbm, freq_ref),
                (source_hbm, source_ref), (biases_hbm, biases_ref),
                (readout_hbm, readout_ref), (weights_hbm, weights_ref),
            )
        )
    ]
    for copy in copies:
        copy.start()
    for copy in copies[:-1]:
        copy.wait()
    fourier_ref[0:3, :] = freq_ref[...]
    small_ref[0:layers, :] = biases_ref[...]
    small_ref[layers : layers + 1, :] = readout_ref[...]
    points = slot_ref.shape[1]
    width = weights_ref.shape[1]
    streams = 5
    off = offsets_ref[...]
    fractions = fractions_ref[...]
    owner_row = owner_ref[...]
    slot = slot_ref[...]
    cells = jnp.concatenate(
        [TILE_SIDE * slot + off[0:1], TILE_SIDE * owner_row + off[1:2], off[2:3]], axis=0
    )
    position = cells.astype(f32) + fractions
    f = jnp.transpose(fourier_ref[...])
    phases = f[:, 0:1] * position[0:1] + f[:, 1:2] * position[1:2] + f[:, 2:3] * position[2:3]
    sin_part, cos_part = sin_cos(phases)
    squared = f[:, 0:1] * f[:, 0:1] + f[:, 1:2] * f[:, 1:2] + f[:, 2:3] * f[:, 2:3]
    freqs = f.shape[0]

    def put(stream, top, bottom):
        for start, value in ((0, top), (freqs, bottom)):
            lanes = pl.ds(stream * points, points)
            hi, lo = split2(value)
            parts_ref[0, pl.ds(start, freqs), lanes] = hi
            parts_ref[0, pl.ds(width + start, freqs), lanes] = lo

    put(0, sin_part, cos_part)
    for k in range(3):
        put(k + 1, cos_part * f[:, k : k + 1], -sin_part * f[:, k : k + 1])
    put(4, -sin_part * squared, -cos_part * squared)

    small_cols = jnp.transpose(small_ref[...])
    col_ref[...] = small_cols
    copies[-1].wait()

    def leave_parts(depth):
        return pltpu.make_async_copy(
            parts_ref.at[depth], parts_hbm.at[depth], out_sems.at[0, depth]
        )

    def leave_pre(depth):
        return pltpu.make_async_copy(pre_ref.at[depth], pre_hbm.at[depth], out_sems.at[1, depth])

    def layer(depth, carry):
        leave_parts(depth).start()
        w_hi, w_lo = split2(weights_ref[depth])
        for k in range(streams):
            lanes = pl.ds(k * points, points)
            h_hi = parts_ref[depth, 0:width, lanes]
            h_lo = parts_ref[depth, width:, lanes]
            z_ref[:, lanes] = dot(w_hi, h_hi) + dot(w_hi, h_lo) + dot(w_lo, h_hi)
        bias = jnp.sum(
            jnp.where(iota(small_cols.shape, 1) == depth, small_cols, 0.0), axis=1, keepdims=True
        )
        bias_ref[...] = bias

        def chunk(c, inner):
            rows = pl.ds(pl.multiple_of(c * FORWARD_ROWS, FORWARD_ROWS), FORWARD_ROWS)
            low_rows = pl.ds(pl.multiple_of(width + c * FORWARD_ROWS, FORWARD_ROWS), FORWARD_ROWS)

            def z_of(k):
                return z_ref[rows, pl.ds(k * points, points)]

            v = jnp.tanh(z_of(0) + bias_ref[rows, :])
            z1, z2, z3, z4 = z_of(1), z_of(2), z_of(3), z_of(4)
            s, _, curve = activations(v, z1, z2, z3, z4)
            for k, (kept, h) in enumerate(
                ((v, v), (z1, s * z1), (z2, s * z2), (z3, s * z3), (z4, curve))
            ):
                lanes = pl.ds(k * points, points)
                pre_ref[depth, rows, lanes] = kept
                hi, lo = split2(h)
                parts_ref[depth + 1, rows, lanes] = hi
                parts_ref[depth + 1, low_rows, lanes] = lo
            return inner

        lax.fori_loop(0, width // FORWARD_ROWS, chunk, 0)
        leave_pre(depth).start()
        return carry

    lax.fori_loop(0, layers, layer, 0)

    def readout_chunk(c, totals):
        rows = pl.ds(pl.multiple_of(c * FORWARD_ROWS, FORWARD_ROWS), FORWARD_ROWS)
        v, z1, z2, z3, z4 = [
            pre_ref[layers - 1, rows, pl.ds(k * points, points)] for k in range(streams)
        ]
        s, _, curve = activations(v, z1, z2, z3, z4)
        r = col_ref[rows, layers : layers + 1]
        hs = (v, s * z1, s * z2, s * z3, curve)
        return tuple(t + jnp.sum(r * h, axis=0, keepdims=True) for t, h in zip(totals, hs))

    zero = tuple(jnp.zeros((1, points), f32) for _ in range(streams))
    out = lax.fori_loop(0, width // FORWARD_ROWS, readout_chunk, zero)
    outputs = jnp.concatenate(list(out) + [jnp.zeros((3, points), f32)], axis=0)
    outputs_ref[...] = outputs

    live = jnp.where(iota((1, points), 1) < live_ref[0, 0], 1.0, 0.0)
    row_index = ((off[0:1] * (TILE_SIDE // 4) + off[1:2] // 4) * tiles + slot).astype(f32)
    lane_index = ((off[1:2] % 4) * TILE_SIDE + off[2:3]).astype(f32)
    comps = [
        row_index, lane_index, fractions[0:1], fractions[1:2], fractions[2:3],
        outputs[1:2], outputs[2:3], outputs[3:4], outputs[4:5], source_ref[...], live,
    ]
    to_owner = owner_row == iota((devices, points), 0)
    ranks = slot_ranks_col(column_of(owner_row), owner_row)
    place = jnp.where(ranks == iota((points, LANES), 1), 1.0, 0.0).astype(bf16)
    spread = jnp.concatenate([jnp.where(to_owner, c, 0.0) for c in comps], axis=0)
    a, b, c = split3(spread)
    packed = dot(a, place) + dot(b, place) + dot(c, place)
    rows_each, lane_groups = request_ref.shape[1], LANES // lanes_each
    for j in range(rows_each):
        total = jnp.zeros((devices, LANES), f32)
        for m in range(lane_groups):
            k = rows_each * m + j
            if k < len(comps):
                part = packed[k * devices : (k + 1) * devices]
                total = total + (pltpu.roll(part, lanes_each * m, 1) if m else part)
        request_ref[:, j, :] = total
    for depth in range(layers):
        leave_parts(depth).wait()
        leave_pre(depth).wait()


def owner_kernel(
    devices, tiles, lanes_each,
    received_ref, window_hi, window_lo,
    response_ref, kept_ref,
    x_ref,
):
    cells = window_hi.shape[1]
    group = LANES // lanes_each
    blocks = devices // group
    slots = blocks * LANES
    rows_each = received_ref.shape[1]
    lane_block = iota((rows_each * group, LANES), 1) // lanes_each
    for j in range(blocks):
        total = None
        for g in range(group):
            part = received_ref[group * j + g]
            moved = jnp.concatenate(
                [
                    pltpu.roll(part, lanes_each * ((g - m) % group), 1) if g != m else part
                    for m in range(group)
                ],
                axis=0,
            )
            total = moved if total is None else jnp.where(lane_block == g, moved, total)
        x_ref[:, j * LANES : (j + 1) * LANES] = total

    step = 2 * LANES
    for start in range(0, slots, step):
        x = x_ref[:, start : start + step]
        rows = x[0:1].astype(jnp.int32)
        place = x[1:2].astype(jnp.int32)
        hot = jnp.where(iota((cells, step), 0) == rows, 1.0, 0.0).astype(bf16)
        found = dot(window_hi[...], hot) + dot(window_lo[...], hot)
        y_mod = place // TILE_SIDE
        z_cell = place % TILE_SIDE
        z_iota = iota((TILE_SIDE, step), 0)
        at_z = (z_iota == z_cell, z_iota == z_cell + 1)
        corner = {}
        for a in range(2):
            parts = [found[a * 160 + TILE_SIDE * j : a * 160 + TILE_SIDE * (j + 1)] for j in range(5)]
            for b in range(2):
                rows_y = jnp.where(y_mod == 0, parts[b], 0.0)
                for j in range(1, 4):
                    rows_y = jnp.where(y_mod == j, parts[j + b], rows_y)
                for c in range(2):
                    corner[a, b, c] = jnp.sum(
                        jnp.where(at_z[c], rows_y, 0.0), axis=0, keepdims=True
                    )
        fr = [x[2:3], x[3:4], x[4:5]]
        w = [(1.0 - t, t) for t in fr]
        sign = (-1.0, 1.0)
        values = [jnp.zeros((1, step), f32) for _ in range(4)]
        for (a, b, c), k in corner.items():
            values[0] = values[0] + w[0][a] * w[1][b] * w[2][c] * k
            values[1] = values[1] + sign[a] * w[1][b] * w[2][c] * k
            values[2] = values[2] + w[0][a] * sign[b] * w[2][c] * k
            values[3] = values[3] + w[0][a] * w[1][b] * sign[c] * k
        du = [x[5:6], x[6:7], x[7:8]]
        lap = x[8:9]
        residual = (
            -(values[0] * lap + (values[1] * du[0] + values[2] * du[1] + values[3] * du[2]))
            - x[9:10]
        )
        scaled = 2.0 * x[10:11] * residual
        zeros = jnp.zeros((4, step), f32)
        answer = jnp.concatenate(values + [zeros], axis=0)
        sub = iota((8, LANES), 0)
        lane_of = iota((8, LANES), 1) // lanes_each
        for j in range(step // LANES):
            block = start // LANES + j
            part = answer[:, j * LANES : (j + 1) * LANES]
            turned = [pltpu.roll(part, lanes_each * k, 1) if k else part for k in range(group)]
            for g in range(group):
                picked = jnp.zeros((8, LANES), f32)
                for c in range(4):
                    picked = jnp.where((sub == c) & (lane_of == c), turned[(c - g) % group], picked)
                response_ref[group * block + g] = jnp.sum(picked, axis=0, keepdims=True)
        kept_ref[:, start : start + step] = jnp.concatenate(
            [x[0:5], -scaled * lap, -scaled * du[0], -scaled * du[1], -scaled * du[2]]
            + [jnp.zeros((7, step), f32)],
            axis=0,
        )


def field_kernel(
    devices, tiles,
    index_ref, kept_ref, field_ref, before_ref, after_ref,
    grad_ref, energy_ref,
    hot_ref, c_hi, c_lo, sum_ref, part_ref,
):
    cells = field_ref.shape[0]
    slots = kept_ref.shape[1]
    plane = (TILE_SIDE // 4) * tiles
    step = 2 * LANES
    for start in range(0, slots, step):
        lanes = slice(start, start + step)
        x = kept_ref[:, lanes]
        rows = x[0:1].astype(jnp.int32)
        place = x[1:2].astype(jnp.int32)
        hot_ref[:, lanes] = jnp.where(iota((cells, step), 0) == rows, 1.0, 0.0).astype(bf16)
        y_mod = place // TILE_SIDE
        z_cell = place % TILE_SIDE
        z_iota = iota((TILE_SIDE, step), 0)
        at_z = (z_iota == z_cell, z_iota == z_cell + 1)
        w = [(1.0 - x[k : k + 1], x[k : k + 1]) for k in (2, 3, 4)]
        g = [x[k : k + 1] for k in (5, 6, 7, 8)]
        sign = (-1.0, 1.0)
        for a in range(2):
            along = []
            for b in range(2):
                pair = []
                for c in range(2):
                    pair.append(
                        g[0] * w[0][a] * w[1][b] * w[2][c]
                        + g[1] * sign[a] * w[1][b] * w[2][c]
                        + g[2] * w[0][a] * sign[b] * w[2][c]
                        + g[3] * w[0][a] * w[1][b] * sign[c]
                    )
                along.append(jnp.where(at_z[0], pair[0], 0.0) + jnp.where(at_z[1], pair[1], 0.0))
            for j in range(5):
                value = jnp.where(y_mod == j, along[0], 0.0) + jnp.where(
                    y_mod == j - 1, along[1], 0.0
                )
                hi, lo = split2(value)
                at = a * 128 + TILE_SIDE * j if j < 4 else 256 + a * TILE_SIDE
                c_hi[at : at + TILE_SIDE, lanes] = hi
                c_lo[at : at + TILE_SIDE, lanes] = lo
    sum_ref[...] = jnp.zeros(sum_ref.shape, f32)
    block = 2 * LANES
    for start in range(0, cells, block):
        hot = hot_ref[start : start + block, :]
        part = dot(hot, c_hi[...], NT) + dot(hot, c_lo[...], NT)
        part_ref[start : start + block, :] = part
    sum_ref[0:cells, :] = part_ref[:, 0:128]
    sum_ref[plane : plane + cells, :] += part_ref[:, 128:256]
    low = slice(0, TILE_SIDE)
    sum_ref[tiles : tiles + cells, low] += part_ref[:, 256 : 256 + TILE_SIDE]
    sum_ref[plane + tiles : plane + tiles + cells, low] += part_ref[
        :, 256 + TILE_SIDE : 256 + 2 * TILE_SIDE
    ]

    me = index_ref[0, 0]
    row = iota((plane, LANES), 0)
    lane = iota((plane, LANES), 1)
    z_inner = (lane % TILE_SIDE) < TILE_SIDE - 1
    first_row = row < tiles
    last_row = row >= plane - tiles
    low_lane = lane < TILE_SIDE
    high_lane = lane >= LANES - TILE_SIDE
    has_after = jnp.where(me < devices - 1, 1.0, 0.0)
    has_before = jnp.where(me > 0, 1.0, 0.0)
    after_mask = jnp.where(last_row & high_lane, has_after, 1.0)
    before_mask = jnp.where(first_row & low_lane, has_before, 1.0)
    next_tile = (row % tiles) < tiles - 1
    prev_tile = (row % tiles) > 0

    def load(x):
        return field_ref[pl.ds(pl.multiple_of(x * plane, plane), plane), :]

    def plane_step(x, energy):
        here = load(x)
        diff_z = jnp.where(z_inner, pltpu.roll(here, LANES - 1, 1) - here, 0.0)
        grad = pltpu.roll(diff_z, 1, 1) - diff_z
        energy = energy + diff_z * diff_z
        above = jnp.concatenate([here[tiles:], after_ref[x]], axis=0)
        up = pltpu.roll(jnp.where(low_lane, above, here), LANES - TILE_SIDE, 1)
        below = jnp.concatenate([before_ref[x], here[: plane - tiles]], axis=0)
        down = pltpu.roll(jnp.where(high_lane, below, here), TILE_SIDE, 1)
        diff_up = (up - here) * after_mask
        diff_down = (here - down) * before_mask
        grad = grad + diff_down - diff_up
        energy = energy + diff_down * diff_down
        first = x == 0
        last = x == TILE_SIDE - 1
        nxt = load(jnp.where(last, 0, x + 1))
        nxt = jnp.where(last, pltpu.roll(nxt, plane - 1, 0), nxt)
        prv = load(jnp.where(first, TILE_SIDE - 1, x - 1))
        prv = jnp.where(first, pltpu.roll(prv, 1, 0), prv)
        diff_next = jnp.where(jnp.logical_not(last) | next_tile, nxt - here, 0.0)
        diff_prev = jnp.where(jnp.logical_not(first) | prev_tile, here - prv, 0.0)
        grad = grad + diff_prev - diff_next
        energy = energy + diff_prev * diff_prev
        at = pl.ds(pl.multiple_of(x * plane, plane), plane)
        grad_ref[at, :] = sum_ref[at, :] + 2.0 * smooth_weight * grad
        return energy

    energy = lax.fori_loop(
        0, TILE_SIDE, plane_step, jnp.zeros((plane, LANES), f32), unroll=4
    )
    energy_ref[...] = jnp.sum(energy, axis=0, keepdims=True)


def prepare_kernel(
    tiles,
    field_ref,
    window_hi, window_lo, first_ref, last_ref,
    padded_ref,
):
    cells = field_ref.shape[0]
    plane = (TILE_SIDE // 4) * tiles
    for x in range(TILE_SIDE):
        first_ref[x] = field_ref[x * plane : x * plane + tiles, :]
        last_ref[x] = field_ref[(x + 1) * plane - tiles : (x + 1) * plane, :]
    padded_ref[0:cells, :] = field_ref[...]
    padded_ref[cells:, :] = jnp.zeros((padded_ref.shape[0] - cells, LANES), f32)
    for a in range(2):
        base = a * plane
        main = jnp.transpose(padded_ref[base : base + cells, :])
        hi, lo = split2(main)
        window_hi[a * 160 : a * 160 + 128, :] = hi
        window_lo[a * 160 : a * 160 + 128, :] = lo
        extra = jnp.transpose(padded_ref[base + tiles : base + tiles + cells, :])[0:TILE_SIDE]
        hi, lo = split2(extra)
        window_hi[a * 160 + 128 : a * 160 + 160, :] = hi
        window_lo[a * 160 + 128 : a * 160 + 160, :] = lo


def backward_kernel(
    devices, layers, lanes_each,
    live_ref, index_ref, owner_row_ref, source_ref, observed_ref, response_ref, energy_ref,
    outputs_ref, readout_ref, weights_hbm, pre_hbm, parts_hbm,
    keep_a_ref, keep_b_ref, send_a_ref, send_b_ref,
    pre_ref, parts_ref, weights_ref, bar_ref, zh_ref, zl_ref, col_ref, cols_ref, sems,
):
    def fetch_pre(k):
        return pltpu.make_async_copy(pre_hbm.at[k], pre_ref.at[k], sems.at[0, k])

    def fetch_parts(k):
        return pltpu.make_async_copy(parts_hbm.at[k], parts_ref.at[k], sems.at[1, k])

    weight_copy = pltpu.make_async_copy(weights_hbm, weights_ref, sems.at[0, layers])
    fetch_pre(layers - 1).start()
    weight_copy.start()
    fetch_parts(layers - 1).start()
    points = owner_row_ref.shape[1]
    width = weights_hbm.shape[1]
    owner_row = owner_row_ref[...]
    ranks = slot_ranks_row(column_of(owner_row), owner_row)
    picked = jnp.where(ranks == iota((lanes_each, points), 0), 1.0, 0.0)
    from_owner = jnp.where(owner_row == iota((devices, points), 0), 1.0, 0.0).astype(bf16)
    a, b, c = split3(jnp.transpose(response_ref[...])[0 : 4 * lanes_each])
    wide = dot(a, from_owner) + dot(b, from_owner) + dot(c, from_owner)
    values = [
        jnp.sum(picked * wide[k * lanes_each : (k + 1) * lanes_each], axis=0, keepdims=True)
        for k in range(4)
    ]
    outputs = outputs_ref[...]
    out = [outputs[k : k + 1] for k in range(5)]
    live = jnp.where(iota((1, points), 1) < live_ref[0, 0], 1.0, 0.0)
    misfit = out[0] - observed_ref[...]
    residual = (
        -(values[0] * out[4] + (values[1] * out[1] + values[2] * out[2] + values[3] * out[3]))
        - source_ref[...]
    )
    scaled = 2.0 * live * residual
    out_grad = [2.0 * data_weight * live * misfit] + [-scaled * values[k] for k in (1, 2, 3, 0)]
    residual_sum = jnp.sum(live * residual * residual, axis=1, keepdims=True)
    misfit_sum = jnp.sum(live * misfit * misfit, axis=1, keepdims=True)
    col_ref[...] = column_of(readout_ref[...])
    cols_ref[...] = jnp.zeros(cols_ref.shape, f32)
    lane8 = iota((ROWS, cols_ref.shape[1]), 1)
    chunks = width // ROWS

    def rows_of(c):
        return pl.ds(pl.multiple_of(c * ROWS, ROWS), ROWS)

    def pre_of(depth, rows):
        return [pre_ref[depth, rows, pl.ds(k * points, points)] for k in range(5)]

    def readout_chunk(c, carry):
        rows = rows_of(c)
        v, z1, z2, z3, z4 = pre_of(layers - 1, rows)
        s, _, curve = activations(v, z1, z2, z3, z4)
        total = out_grad[0] * v + out_grad[1] * (s * z1) + out_grad[2] * (s * z2)
        total = total + out_grad[3] * (s * z3) + out_grad[4] * curve
        grad = jnp.sum(total, axis=1, keepdims=True)
        cols_ref[rows, :] += jnp.where(lane8 == layers, grad, 0.0)
        r = col_ref[rows, :]
        for k in range(5):
            bar_ref[rows, pl.ds(k * points, points)] = r * out_grad[k]
        return carry

    fetch_pre(layers - 1).wait()
    lax.fori_loop(0, chunks, readout_chunk, 0)
    weight_copy.wait()
    mine = index_ref[0, 0] % 2
    half = layers // 2

    def layer(step, carry):
        depth = layers - 1 - step
        before = jnp.maximum(depth - 1, 0)

        @pl.when(depth > 0)
        def _():
            fetch_pre(before).start()
            fetch_parts(before).start()

        def bars(c, inner):
            rows = rows_of(c)
            v, z1, z2, z3, z4 = pre_of(depth, rows)
            b = [bar_ref[rows, pl.ds(k * points, points)] for k in range(5)]
            s = 1.0 - v * v
            q = z1 * z1 + z2 * z2 + z3 * z3
            slope = b[1] * z1 + b[2] * z2 + b[3] * z3
            v4c = 4.0 * v * b[4]
            z_bar = [
                s
                * (
                    b[0]
                    - 2.0 * v * slope
                    + b[4] * (q * (4.0 * v * v - 2.0 * s) - 2.0 * v * z4)
                ),
                s * (b[1] - v4c * z1),
                s * (b[2] - v4c * z2),
                s * (b[3] - v4c * z3),
                s * b[4],
            ]
            grad = jnp.sum(z_bar[0], axis=1, keepdims=True)
            cols_ref[rows, :] += jnp.where(lane8 == depth, grad, 0.0)
            for k in range(5):
                lanes = pl.ds(k * points, points)
                hi, lo = split2(z_bar[k])
                zh_ref[rows, lanes] = hi
                zl_ref[rows, lanes] = lo
            return inner

        lax.fori_loop(0, chunks, bars, 0, unroll=2)
        fetch_parts(depth).wait()
        h_hi, h_lo = parts_ref[depth, 0:width], parts_ref[depth, width:]
        z_hi, z_lo = zh_ref[...], zl_ref[...]
        grad = dot(z_hi, h_hi, NT) + dot(z_hi, h_lo, NT) + dot(z_lo, h_hi, NT)
        upper = (depth >= half).astype(jnp.int32)
        part = width // 2
        at = pl.ds(pl.multiple_of((depth - upper * half) * part, part), part)

        @pl.when(mine == upper)
        def _():
            keep_a_ref[at, :] = grad[:part]
            keep_b_ref[at, :] = grad[part:]

        @pl.when(mine != upper)
        def _():
            send_a_ref[at, :] = grad[:part]
            send_b_ref[at, :] = grad[part:]

        @pl.when(depth > 0)
        def _():
            w_hi, w_lo = split2(jnp.transpose(weights_ref[depth]))
            for k in range(5):
                lanes = pl.ds(k * points, points)
                z_hi = zh_ref[:, lanes]
                bar_ref[:, lanes] = dot(w_hi, z_hi) + dot(w_hi, zl_ref[:, lanes]) + dot(w_lo, z_hi)
            fetch_pre(before).wait()

        return carry

    lax.fori_loop(0, layers, layer, 0)
    small = jnp.transpose(cols_ref[...])
    lane = iota((1, width), 1)
    count = jnp.full((1, 1), live_ref[0, 0], jnp.int32).astype(f32)
    last = jnp.where(lane == 0, residual_sum, 0.0) + jnp.where(lane == 1, misfit_sum, 0.0)
    energy = jnp.sum(energy_ref[...], axis=1, keepdims=True)
    last = last + jnp.where(lane == 2, count, 0.0) + jnp.where(lane == 3, energy, 0.0)
    small = jnp.where(iota(small.shape, 0) == small.shape[0] - 1, last, small)
    keep_b_ref[half * width // 2 :, :] = small
    send_b_ref[half * width // 2 :, :] = small


def finish_kernel(cells_total, sums_ref, bias_ref, readout_ref, losses_ref, scale_ref):
    layers = bias_ref.shape[0]
    width = bias_ref.shape[1]
    sums = sums_ref[...]
    lane = iota((1, width), 1)
    last = sums[7:8]
    count = jnp.sum(jnp.where(lane == 2, last, 0.0), axis=1, keepdims=True)
    scale = jnp.broadcast_to(1.0 / count, (1, width))
    bias_ref[...] = sums[:layers] * scale
    readout_ref[...] = sums[layers : layers + 1] * scale
    energy = jnp.sum(jnp.where(lane == 3, last, 0.0), axis=1, keepdims=True)
    losses = jnp.where(lane == 2, energy / cells_total, last * scale)
    losses_ref[...] = losses[:, 0:3]
    scale_ref[...] = scale


def vmem():
    return pl.BlockSpec(memory_space=pltpu.VMEM)


def smem():
    return pl.BlockSpec(memory_space=pltpu.SMEM)


def hbm():
    return pl.BlockSpec(memory_space=pltpu.HBM)


def call(kernel, name, specs, out_shapes, scratch, flops, limit, outs=None):
    return pl.pallas_call(
        kernel,
        name=name,
        out_shape=out_shapes,
        in_specs=specs,
        out_specs=outs or jax.tree.map(lambda _: vmem(), out_shapes),
        scratch_shapes=scratch,
        compiler_params=pltpu.CompilerParams(vmem_limit_bytes=min(limit << 20, 67043328)),
        cost_estimate=pl.CostEstimate(flops=flops, bytes_accessed=1 << 20, transcendentals=0),
    )


def shape(*dims, dtype=f32):
    return jax.ShapeDtypeStruct(dims, dtype)


def on_device(
    conductivity, owner_rank, tile_slot, offsets, fractions, source, observed, live_count,
    fourier, weights, biases, readout,
):
    devices = lax.axis_size(AXES)
    index = lax.axis_index(AXES)
    points = tile_slot.shape[0]
    tiles = conductivity.shape[0]
    layers, width = biases.shape
    capacity = (2 * points + devices - 1) // devices + 1
    lanes_each = 1 << (capacity - 1).bit_length()
    lanes_each = max(lanes_each, 2 * LANES // devices)
    rows_each = 1 << (-(-11 * lanes_each // LANES) - 1).bit_length()
    slots = devices * lanes_each
    cells = conductivity.size // LANES
    plane = (TILE_SIDE // 4) * tiles
    wide = 5 * points

    live, place = live_count.reshape(1, 1), index.reshape(1, 1)
    owner_row = owner_rank.reshape(1, points)
    source_row = source.reshape(1, points)
    readout_row = readout.reshape(1, width)
    field = conductivity.reshape(tiles, cells // tiles, LANES).transpose(1, 0, 2)
    field = field.reshape(cells, LANES)

    request, outputs, pre, parts = call(
        functools.partial(forward_kernel, devices, layers, tiles, lanes_each),
        "forward",
        [smem()] + [hbm()] * 9,
        (
            shape(devices, rows_each, LANES), shape(8, points),
            shape(layers, width, wide), shape(layers, 2 * width, wide, dtype=bf16),
        ),
        [
            pltpu.VMEM((layers, width, wide), f32),
            pltpu.VMEM((layers + 1, 2 * width, wide), bf16),
            pltpu.VMEM((layers, width, width), f32),
            pltpu.VMEM((width, wide), f32),
            pltpu.VMEM((width, 8), f32),
            pltpu.VMEM((width, 1), f32),
            pltpu.VMEM((1, points), jnp.int32),
            pltpu.VMEM((1, points), jnp.int32),
            pltpu.VMEM((3, points), jnp.int32),
            pltpu.VMEM((3, points), f32),
            pltpu.VMEM((1, points), f32),
            pltpu.VMEM((8, fourier.shape[0]), f32),
            pltpu.VMEM((8, width), f32),
            pltpu.VMEM((3, fourier.shape[0]), f32),
            pltpu.VMEM((layers, width), f32),
            pltpu.VMEM((1, width), f32),
            pltpu.SemaphoreType.DMA((9,)),
            pltpu.SemaphoreType.DMA((2, layers)),
        ],
        6 * 2 * layers * width * width * wide,
        FORWARD_LIMIT,
        outs=(vmem(), vmem(), hbm(), hbm()),
    )(
        live, owner_row, tile_slot.reshape(1, points), offsets, fractions,
        source_row, fourier.T, weights, biases, readout_row,
    )
    received = lax.all_to_all(request, AXES, split_axis=0, concat_axis=0, tiled=True)

    field_here, _ = lax.optimization_barrier((field, outputs))
    window_hi, window_lo, first, last = call(
        functools.partial(prepare_kernel, tiles),
        "prepare",
        [vmem()],
        (
            shape(320, cells, dtype=bf16), shape(320, cells, dtype=bf16),
            shape(TILE_SIDE, tiles, LANES), shape(TILE_SIDE, tiles, LANES),
        ),
        [pltpu.VMEM((cells + 2 * plane, LANES), f32)],
        FILL,
        PREPARE_LIMIT,
    )(field_here)
    up = [(i, i + 1) for i in range(devices - 1)]
    down = [(j, i) for i, j in up]
    before = lax.ppermute(last, AXES, up)
    after = lax.ppermute(first, AXES, down)
    received, before, after = lax.optimization_barrier((received, before, after))

    response, kept = call(
        functools.partial(owner_kernel, devices, tiles, lanes_each),
        "lookup",
        [vmem()] * 3,
        (shape(devices, 1, LANES), shape(16, slots)),
        [pltpu.VMEM((16, slots), f32)],
        2 * 640 * cells * slots,
        LOOKUP_LIMIT,
    )(received, window_hi, window_lo)
    answered = lax.all_to_all(response, AXES, split_axis=0, concat_axis=0, tiled=True)
    grad, energy = call(
        functools.partial(field_kernel, devices, tiles),
        "field",
        [smem()] + [vmem()] * 4,
        (shape(cells, LANES), shape(1, LANES)),
        [
            pltpu.VMEM((cells, slots), bf16),
            pltpu.VMEM((320, slots), bf16),
            pltpu.VMEM((320, slots), bf16),
            pltpu.VMEM((cells + 2 * plane, LANES), f32),
            pltpu.VMEM((cells, 320), f32),
        ],
        FILL,
        SPREAD_LIMIT,
    )(place, kept, field_here, before, after)
    answered, grad = lax.optimization_barrier((answered, grad))

    part_rows = layers * width // 4
    keep_a, keep_b, send_a, send_b = call(
        functools.partial(backward_kernel, devices, layers, lanes_each),
        "backward",
        [smem()] * 2 + [vmem()] * 7 + [hbm()] * 3,
        tuple(shape(rows, width) for rows in (part_rows, part_rows + 8) * 2),
        [
            pltpu.VMEM((layers, width, wide), f32),
            pltpu.VMEM((layers, 2 * width, wide), bf16),
            pltpu.VMEM((layers, width, width), f32),
            pltpu.VMEM((width, wide), f32),
            pltpu.VMEM((width, wide), bf16),
            pltpu.VMEM((width, wide), bf16),
            pltpu.VMEM((width, 1), f32),
            pltpu.VMEM((width, 8), f32),
            pltpu.SemaphoreType.DMA((2, layers + 1)),
        ],
        12 * 2 * layers * width * width * wide,
        BACKWARD_LIMIT,
    )(
        live, place, owner_row, source_row, observed.reshape(1, points),
        answered.reshape(devices, LANES), energy, outputs, readout_row, weights, pre, parts,
    )

    even = [1 << k for k in range(devices.bit_length() - 1)]
    odd = list(even)
    for k in range(1, len(odd) - 1, 2):
        odd[k], odd[k + 1] = odd[k + 1], odd[k]

    def exchange(value, step):
        bits = (even[step], odd[step])
        return lax.ppermute(value, AXES, [(i, i ^ bits[i % 2]) for i in range(devices)])

    def upper_of(step):
        bit = jnp.where(index % 2 == 1, odd[step], even[step])
        return (index & bit) != 0

    main = [keep_a + exchange(send_a, 0), keep_b + exchange(send_b, 0)]
    main[1], extra = main[1][:part_rows], main[1][part_rows:]
    for step in range(1, len(even)):
        half = main[0].shape[0] // 2
        upper = upper_of(step)
        outgoing = [jnp.where(upper, m[:half], m[half:]) for m in main]
        outgoing[1] = jnp.concatenate([outgoing[1], extra], axis=0)
        arrived = [exchange(value, step) for value in outgoing]
        main = [jnp.where(upper, m[half:], m[:half]) + a[:half] for m, a in zip(main, arrived)]
        extra = extra + arrived[1][half:]
    for step in reversed(range(len(even))):
        upper = upper_of(step)
        outgoing = list(main)
        if step == len(even) - 1:
            outgoing[1] = jnp.concatenate([main[1], extra], axis=0)
        arrived = [exchange(value, step) for value in outgoing]
        if step == len(even) - 1:
            rows = main[1].shape[0]
            arrived[1], extra = arrived[1][:rows], arrived[1][rows:]
        main = [
            jnp.concatenate([jnp.where(upper, a, m), jnp.where(upper, m, a)], axis=0)
            for m, a in zip(main, arrived)
        ]
    bias_grad, readout_grad, losses, scale = call(
        functools.partial(finish_kernel, float(devices * conductivity.size)),
        "finish",
        [vmem()],
        (shape(layers, width), shape(1, width), shape(1, 3), shape(1, width)),
        [],
        FILL,
        4,
    )(extra)
    weight_grad = scale * jnp.concatenate(
        [m.reshape(layers, width // 2, width) for m in main], axis=1
    )
    conductivity_grad = grad.reshape(cells // tiles, tiles, LANES).transpose(1, 0, 2)
    return (
        conductivity_grad.reshape(conductivity.shape),
        weight_grad,
        bias_grad,
        readout_grad.reshape(readout.shape),
        losses.reshape(3),
    )


def solution(mesh):
    in_specs = (
        P(AXES, None), P(AXES, None), P(AXES), P(None, AXES), P(None, AXES), P(AXES), P(AXES),
        P(AXES), P(), P(), P(), P(),
    )
    out_specs = (P(AXES, None), P(), P(), P(), P())
    return jax.shard_map(
        on_device, mesh=mesh, in_specs=in_specs, out_specs=out_specs, check_vma=False
    )
```
